32 devices in a mesh: inst: 1 (over z), dev: 4 (over y), side: 8 (over x, core).
Axes of the slice: x: 4, y: 4, z: 1, core: 2. Of those that a mesh axis runs over, the one named last changes fastest.
The devices are a block of a 4x4x8 slice.
Arguments:
- hidden: bfloat16 [512, 3584], P(('inst', 'dev'))
- cache_len: int32 [512], P(('inst', 'dev'))
- k_cache: bfloat16 [1, 512, 8, 64, 256], P(None, ('inst', 'dev'))
- v_cache: bfloat16 [1, 512, 8, 64, 256], P(None, ('inst', 'dev'))
- w_q: bfloat16 [1, 3584, 4096], replicated
- w_kv: bfloat16 [1, 3584, 4096], replicated
- w_o: bfloat16 [1, 4096, 3584], replicated
- attn_gain: float32 [1, 3584], replicated
- ffn_gain: float32 [1, 3584], replicated
- w_gate: bfloat16 [1, 3584, 14336], P(None, None, 'dev')
- w_up: bfloat16 [1, 3584, 14336], P(None, None, 'dev')
- w_down: bfloat16 [1, 14336, 3584], P(None, 'dev')
Outputs:
- output: bfloat16 [512, 3584], P(('inst', 'dev', 'side'))
All inputs are finite; a program needn't handle non-finite values.
Results may differ from the reference program's by a relative error of at most 0.0123053.
Values are sent between devices in bfloat16 or wider.
A program may use at most 768 MiB of HBM per device.

```python
import math
import jax
import jax.numpy as jnp
from jax import lax

D = 3584
FF = 14336
HEADS = 16
KV_HEADS = 8
HEAD = 256
SEQ = 64
LAYERS = 1
BATCH = 512

EPS = 1e-5
ROPE_BASE = 10000.0
KEY_STD = math.sqrt(1.5 * math.log(SEQ))
GROUP = HEADS // KV_HEADS


def setup_inputs(seed: int = 0, part: int = 0) -> dict:
    base_key = jax.random.key(seed)
    part_key = jax.random.fold_in(base_key, part)
    shared = jax.random.split(base_key, 8)
    local = jax.random.split(part_key, 6)
    hidden = jax.random.normal(local[0], (BATCH, D), jnp.float32)
    cache_len = jax.random.randint(local[1], (BATCH,), 1, SEQ + 1, dtype=jnp.int32)
    cache_len = cache_len.at[0].set(SEQ).at[1].set(1)
    cache_shape = (LAYERS, BATCH, KV_HEADS, SEQ, HEAD)
    mean_shape = (LAYERS, BATCH, KV_HEADS, 1, HEAD)
    pos_ramp = (2.0 * jnp.arange(SEQ, dtype=jnp.float32) / SEQ - 1.0).reshape(1, 1, 1, SEQ, 1)
    k_cache = KEY_STD * jax.random.normal(local[2], cache_shape, jnp.float32)
    v_cache = (jax.random.normal(local[3], cache_shape, jnp.float32)
               + 0.7 * jax.random.normal(local[4], mean_shape, jnp.float32)
               + 0.7 * pos_ramp * jax.random.normal(local[5], mean_shape, jnp.float32))
    kv_cols = KV_HEADS * HEAD
    col_scale = jnp.concatenate([jnp.full((kv_cols,), KEY_STD, jnp.float32), jnp.full((kv_cols,), 2.0, jnp.float32)])
    w_q = jax.random.normal(shared[0], (LAYERS, D, HEADS * HEAD), jnp.float32) * D ** -0.5
    w_kv = jax.random.normal(shared[1], (LAYERS, D, 2 * kv_cols), jnp.float32) * (D ** -0.5) * col_scale
    w_o = jax.random.normal(shared[2], (LAYERS, HEADS * HEAD, D), jnp.float32) * (HEADS * HEAD) ** -0.5
    attn_gain = jax.random.uniform(shared[3], (LAYERS, D), jnp.float32, 0.5, 1.5)
    ffn_gain = jax.random.uniform(shared[4], (LAYERS, D), jnp.float32, 0.5, 1.5)
    w_gate = jax.random.normal(shared[5], (LAYERS, D, FF), jnp.float32) * D ** -0.5
    w_up = jax.random.normal(shared[6], (LAYERS, D, FF), jnp.float32) * D ** -0.5
    w_down = jax.random.normal(shared[7], (LAYERS, FF, D), jnp.float32) * (1.5 * FF ** -0.5)
    return {
        'hidden': hidden.astype(jnp.bfloat16),
        'cache_len': cache_len,
        'k_cache': k_cache.astype(jnp.bfloat16),
        'v_cache': v_cache.astype(jnp.bfloat16),
        'w_q': w_q.astype(jnp.bfloat16),
        'w_kv': w_kv.astype(jnp.bfloat16),
        'w_o': w_o.astype(jnp.bfloat16),
        'attn_gain': attn_gain,
        'ffn_gain': ffn_gain,
        'w_gate': w_gate.astype(jnp.bfloat16),
        'w_up': w_up.astype(jnp.bfloat16),
        'w_down': w_down.astype(jnp.bfloat16),
    }


def rms_norm(rows, gain):
    rows_f = rows.astype(jnp.float32)
    inv_rms = lax.rsqrt(jnp.mean(rows_f * rows_f, axis=-1, keepdims=True) + EPS)
    return (rows_f * inv_rms * gain).astype(jnp.bfloat16)


def rotary(vecs, positions):
    half_dim = vecs.shape[-1] // 2
    freqs = ROPE_BASE ** (-jnp.arange(half_dim, dtype=jnp.float32) / half_dim)
    angle = positions.astype(jnp.float32)[:, None, None] * freqs
    cos_part = jnp.cos(angle)
    sin_part = jnp.sin(angle)
    first = vecs[..., :half_dim]
    second = vecs[..., half_dim:]
    return jnp.concatenate([first * cos_part - second * sin_part, second * cos_part + first * sin_part], axis=-1)


def attend_one(operands):
    q_row, k_new, v_new, k_seq, v_seq, length = operands
    scale = HEAD ** -0.5
    q_f = q_row.astype(jnp.float32)
    scores = jnp.einsum('kgd,ksd->kgs', q_f, k_seq.astype(jnp.float32)) * scale
    valid = jnp.arange(SEQ)[None, None, :] < length
    scores = jnp.where(valid, scores, -1e30)
    self_score = jnp.einsum('kgd,kd->kg', q_f, k_new.astype(jnp.float32)) * scale
    row_max = jnp.maximum(jnp.max(scores, axis=-1), self_score)
    exp_scores = jnp.exp(scores - row_max[..., None])
    self_exp = jnp.exp(self_score - row_max)
    total_exp = jnp.sum(exp_scores, axis=-1) + self_exp
    mixed = jnp.einsum('kgs,ksd->kgd', exp_scores.astype(jnp.bfloat16).astype(jnp.float32), v_seq.astype(jnp.float32))
    mixed = mixed + self_exp.astype(jnp.bfloat16).astype(jnp.float32)[..., None] * v_new.astype(jnp.float32)[:, None, :]
    return (mixed / total_exp[..., None]).astype(jnp.bfloat16)


def reference(hidden, cache_len, k_cache, v_cache, w_q, w_kv, w_o, attn_gain, ffn_gain, w_gate, w_up, w_down):
    def layer_step(x_cur, per_layer):
        q_weight, kv_weight, o_weight, gain_attn, gain_ffn, gate_weight, up_weight, down_weight, k_layer, v_layer = per_layer
        normed = rms_norm(x_cur, gain_attn)
        q_all = jnp.dot(normed, q_weight, preferred_element_type=jnp.float32).reshape(BATCH, HEADS, HEAD)
        kv_all = jnp.dot(normed, kv_weight, preferred_element_type=jnp.float32).reshape(BATCH, 2, KV_HEADS, HEAD)
        q_rows = rotary(q_all, cache_len).astype(jnp.bfloat16).reshape(BATCH, KV_HEADS, GROUP, HEAD)
        k_new = rotary(kv_all[:, 0], cache_len).astype(jnp.bfloat16)
        v_new = kv_all[:, 1].astype(jnp.bfloat16)
        mixed = lax.map(attend_one, (q_rows, k_new, v_new, k_layer, v_layer, cache_len))
        attn_out = jnp.dot(mixed.reshape(BATCH, HEADS * HEAD), o_weight, preferred_element_type=jnp.float32)
        x_mid = (x_cur.astype(jnp.float32) + attn_out).astype(jnp.bfloat16)
        h_rows = rms_norm(x_mid, gain_ffn)
        gate = jnp.dot(h_rows, gate_weight, preferred_element_type=jnp.float32)
        up_proj = jnp.dot(h_rows, up_weight, preferred_element_type=jnp.float32)
        act_rows = (jax.nn.silu(gate) * up_proj).astype(jnp.bfloat16)
        y_rows = jnp.dot(act_rows, down_weight, preferred_element_type=jnp.float32).astype(jnp.bfloat16)
        x_next = (x_mid.astype(jnp.float32) + y_rows.astype(jnp.float32)).astype(jnp.bfloat16)
        return x_next, None

    x_out, _ = lax.scan(layer_step, hidden, (w_q, w_kv, w_o, attn_gain, ffn_gain, w_gate, w_up, w_down, k_cache, v_cache))
    return x_out
```

```python
import functools

import jax
import jax.numpy as jnp
import numpy as np
from jax import lax
from jax.experimental import pallas as pl
from jax.experimental.pallas import tpu as pltpu
from jax.sharding import PartitionSpec as P

EPS = 1e-5
ROPE_BASE = 10000.0
MESH = pl.DeviceIdType.MESH
F32 = jnp.float32
BF16 = jnp.bfloat16
COL = 256
CORES = 2
NEG = -1e30


def dot(lhs, rhs):
    return jnp.dot(lhs, rhs, preferred_element_type=F32)


def rms(rows, gain):
    rows_f = rows.astype(F32)
    inv = lax.rsqrt(jnp.mean(rows_f * rows_f, axis=-1, keepdims=True) + EPS)
    return (rows_f * inv * gain).astype(BF16)


def pair_blocks(first, second):
    rows, n = first.shape
    both = jnp.concatenate([first.reshape(rows // 8, 8, n), second.reshape(rows // 8, 8, n)], axis=1)
    return both.reshape(2 * rows, n)


def layer_kernel(n_dev, n_side,
                 x_hbm, len_hbm, freq_hbm, k_hbm, v_hbm, wq_hbm, wkv_hbm, wo_hbm, again_hbm, fgain_hbm,
                 wg_hbm, wu_hbm, wd_hbm, out_hbm,
                 act, lens, freqs, again, fgain, xres, wa, kbuf, vbuf, wo, wg, wu,
                 yb, qa, sb, pb, ob, osend, og, pp, precv, x1g, u, r1, r2, r3, fin, finr,
                 in_sem, w_sem, kv_sem, wo_sem, gu_sem, wd_sem, out_sem,
                 a2a_send, a2a_recv, pp_send, pp_recv, ag_send, ag_recv, u_send, u_recv,
                 rs_send, rs_recv, fin_send, fin_recv):
    dev = lax.axis_index('dev')
    side = lax.axis_index('side')
    n_x = n_side // CORES
    chip = lax.div(side, CORES)
    core = lax.rem(side, CORES)
    mate = {'side': CORES * chip + 1 - core}
    seqs, width = act.shape
    head = COL
    q_cols = osend.shape[1]
    half = width // 2
    rows = xres.shape[0]
    n_col = half // COL
    kv_half = wkv_hbm.shape[2] // 2
    prow, pcol = wa.shape[0], wa.shape[1]

    def on_x(r):
        return {'side': CORES * lax.rem(chip + r, n_x) + core}

    def on_y(r):
        return {'dev': lax.rem(dev + r + n_dev, n_dev)}

    barrier = pltpu.get_barrier_semaphore()
    peers = [mate] + [on_x(r) for r in range(1, n_x)] + [on_y(1), on_y(-1)]
    for peer in peers:
        pl.semaphore_signal(barrier, inc=1, device_id=peer, device_id_type=MESH)

    def cols(start, size):
        return pl.ds(pl.multiple_of(start, 128), size)

    def load(src, dst, sem, priority=1):
        pltpu.make_async_copy(src, dst, sem).start(priority=priority)

    def landed(dst, sem):
        pltpu.make_async_copy(dst, dst, sem).wait()

    mine = cols(core * half, half)
    other = cols((1 - core) * half, half)
    my_rows = pl.ds(pl.multiple_of(chip * rows, rows), rows)

    load(x_hbm, act, in_sem.at[0])
    load(len_hbm, lens, in_sem.at[1])
    load(freq_hbm, freqs, in_sem.at[2])
    load(again_hbm, again, in_sem.at[3])
    load(fgain_hbm, fgain, in_sem.at[4])
    load(x_hbm.at[my_rows, mine], xres, in_sem.at[5])

    def w_slot(j):
        return wa.at[:, :, j * COL:(j + 1) * COL]

    load(wq_hbm.at[:, :, cols(side * q_cols, COL)], w_slot(0), w_sem.at[0])
    load(wq_hbm.at[:, :, cols(side * q_cols + COL, COL)], w_slot(1), w_sem.at[1])
    load(wkv_hbm.at[:, :, cols(side * head, COL)], w_slot(2), w_sem.at[2])
    load(wkv_hbm.at[:, :, cols(kv_half + side * head, COL)], w_slot(3), w_sem.at[3])
    load(k_hbm.at[:, side], kbuf, kv_sem.at[0])
    load(v_hbm.at[:, side], vbuf, kv_sem.at[1])
    for r in range(n_x):
        src_chip = lax.rem(chip + n_x - r, n_x)
        load(wo_hbm.at[CORES * src_chip + core], wo.at[r], wo_sem.at[r])
    for j in range(n_col - 1):
        part = slice(j * COL, (j + 1) * COL)
        load(wg_hbm.at[:, :, cols(core * half + j * COL, COL)], wg.at[:, :, part], gu_sem.at[0, j])
        load(wu_hbm.at[:, :, cols(core * half + j * COL, COL)], wu.at[:, :, part], gu_sem.at[1, j])

    for i, ref in enumerate((act, lens, freqs, again, fgain, xres)):
        landed(ref, in_sem.at[i])
    row_id = lax.broadcasted_iota(jnp.int32, (seqs, seqs), 0)
    col_id = lax.broadcasted_iota(jnp.int32, (seqs, seqs), 1)
    wide = jnp.broadcast_to(lens[...].astype(F32), (seqs, seqs))
    len_col = jnp.sum(jnp.where(row_id == col_id, wide, 0.0), axis=1, keepdims=True)
    angle = len_col * freqs[...]
    cos_part = jnp.cos(angle)
    sin_part = jnp.sin(angle)

    def rotate(vecs):
        first, second = vecs[:, :head // 2], vecs[:, head // 2:]
        return jnp.concatenate([first * cos_part - second * sin_part, second * cos_part + first * sin_part], axis=1)

    @pl.loop(0, seqs // 16)
    def _(i):
        block = pl.ds(pl.multiple_of(i * 16, 16), 16)
        act[block, :] = rms(act[block, :], again[...])

    @pl.loop(0, 4)
    def _(j):
        landed(w_slot(0), w_sem.at[j])
        w = wa[:, :, cols(j * COL, COL)].reshape(prow * pcol, COL)
        yb[j] = dot(act[...], w)

    q0 = rotate(yb[0]).astype(BF16).astype(F32)
    q1 = rotate(yb[1]).astype(BF16).astype(F32)
    k_new = rotate(yb[2]).astype(BF16).astype(F32)
    v_new = yb[3].astype(BF16).astype(F32)
    qa[...] = pair_blocks(q0, q1).astype(BF16)
    scale = head ** -0.5
    self0 = jnp.sum(q0 * k_new, axis=1, keepdims=True)
    self1 = jnp.sum(q1 * k_new, axis=1, keepdims=True)
    self_score = pair_blocks(self0, self1) * scale
    len_rows = pair_blocks(len_col, len_col).astype(jnp.int32)

    span = kbuf.shape[1]
    keys = 8 * span
    landed(kbuf, kv_sem.at[0])
    for b in range(seqs // 8):
        k_blk = kbuf[8 * b:8 * b + 8].reshape(keys, head)
        sb[16 * b:16 * b + 16, :] = lax.dot_general(
            qa[16 * b:16 * b + 16, :], k_blk, (((1,), (1,)), ((), ())), preferred_element_type=F32)
    row = lax.broadcasted_iota(jnp.int32, (2 * seqs, keys), 0)
    key = lax.broadcasted_iota(jnp.int32, (2 * seqs, keys), 1)
    offset = key - lax.rem(row, 8) * span
    valid = (offset >= 0) & (offset < len_rows)
    scores = jnp.where(valid, sb[...] * scale, NEG)
    row_max = jnp.maximum(jnp.max(scores, axis=1, keepdims=True), self_score)
    exp_scores = jnp.exp(scores - row_max)
    self_exp = jnp.exp(self_score - row_max)
    total = jnp.sum(exp_scores, axis=1, keepdims=True) + self_exp
    pb[...] = exp_scores.astype(BF16)
    landed(vbuf, kv_sem.at[1])
    for b in range(seqs // 8):
        v_blk = vbuf[8 * b:8 * b + 8].reshape(keys, head)
        ob[16 * b:16 * b + 16, :] = dot(pb[16 * b:16 * b + 16, :], v_blk)
    mixed = ob[...] + self_exp.astype(BF16).astype(F32) * pair_blocks(v_new, v_new)
    mixed = (mixed / total).reshape(seqs // 8, 16, head)
    osend[:, :head] = mixed[:, :8].reshape(seqs, head).astype(BF16)
    osend[:, head:] = mixed[:, 8:].reshape(seqs, head).astype(BF16)

    last = (n_col - 1) * COL
    load(wg_hbm.at[:, :, cols(core * half + last, COL)], kbuf.at[0:prow], gu_sem.at[0, n_col - 1])
    load(wu_hbm.at[:, :, cols(core * half + last, COL)], vbuf.at[0:prow], gu_sem.at[1, n_col - 1])
    for j in range(n_col):
        load(wd_hbm.at[:, :, cols(core * half + j * COL, COL)], wa.at[:, :, j * COL:(j + 1) * COL], wd_sem.at[j])

    pl.semaphore_wait(barrier, len(peers))

    def send(src, dst, send_sem, recv_sem, where):
        pltpu.make_async_remote_copy(src, dst, send_sem, recv_sem, device_id=where, device_id_type=MESH).start()

    def arrived(dst, sem):
        pltpu.make_async_copy(dst, dst, sem).wait()

    for r in range(1, n_x):
        there = lax.rem(chip + r, n_x)
        send(osend.at[pl.ds(pl.multiple_of(there * rows, rows), rows)], og.at[r], a2a_send.at[r], a2a_recv.at[r], on_x(r))

    @pl.loop(0, 2 * n_col)
    def _(j):
        pp[j] = jnp.zeros_like(pp[0])

    steps = [0, 1] + [r for r in range(n_x - 1, 1, -1)]
    for r in steps:
        landed(wo.at[r], wo_sem.at[r])
        if r == 0:
            o_rows = osend[my_rows, :]
        else:
            arrived(og.at[r], a2a_recv.at[r])
            o_rows = og[r]

        def project(start):
            @pl.loop(0, n_col)
            def _(j, o_rows=o_rows, r=r):
                pp[start + j] += dot(o_rows, wo[r, :, cols((start + j) * COL, COL)])

        project((1 - core) * n_col)
        if r == steps[-1]:
            send(pp.at[pl.ds((1 - core) * n_col, n_col)], precv, pp_send.at[0], pp_recv.at[0], mate)
        project(core * n_col)
    arrived(precv, pp_recv.at[0])

    @pl.loop(0, n_col)
    def _(j):
        part = cols(j * COL, COL)
        full = cols(core * half + j * COL, COL)
        summed = pp[core * n_col + j] + precv[j]
        x1g[pl.ds(pl.multiple_of(dev * rows, rows), rows), full] = (xres[:, part].astype(F32) + summed).astype(BF16)

    def piece(owner, start, size):
        owner_rows = pl.ds(pl.multiple_of(lax.rem(owner + 2 * n_dev, n_dev) * rows, rows), rows)
        return x1g.at[owner_rows, cols(core * half + start, size)]

    def their_piece(owner, start, size):
        owner_rows = pl.ds(pl.multiple_of(lax.rem(owner + 2 * n_dev, n_dev) * rows, rows), rows)
        return x1g.at[owner_rows, cols((1 - core) * half + start, size)]

    quarter = half // 2
    own = piece(dev, 0, half)
    send(own, own, ag_send.at[0], ag_recv.at[0], on_y(1))
    send(own, own, ag_send.at[1], ag_recv.at[1], on_y(-1))
    send(own, own, ag_send.at[4], ag_recv.at[4], mate)
    below = piece(dev - 1, 0, half)
    arrived(below, ag_recv.at[0])
    below_a = piece(dev - 1, 0, quarter)
    send(below_a, below_a, ag_send.at[2], ag_recv.at[2], on_y(1))
    send(below, below, ag_send.at[5], ag_recv.at[5], mate)
    above = piece(dev + 1, 0, half)
    arrived(above, ag_recv.at[1])
    above_b = piece(dev + 1, quarter, quarter)
    send(above_b, above_b, ag_send.at[3], ag_recv.at[3], on_y(-1))
    send(above, above, ag_send.at[6], ag_recv.at[6], mate)
    far_a, far_b = piece(dev + 2, 0, quarter), piece(dev + 2, quarter, quarter)
    arrived(far_a, ag_recv.at[2])
    send(far_a, far_a, ag_send.at[7], ag_recv.at[7], mate)
    arrived(far_b, ag_recv.at[3])
    send(far_b, far_b, ag_send.at[8], ag_recv.at[8], mate)
    arrived(their_piece(dev, 0, half), ag_recv.at[4])
    arrived(their_piece(dev - 1, 0, half), ag_recv.at[5])
    arrived(their_piece(dev + 1, 0, half), ag_recv.at[6])
    arrived(their_piece(dev + 2, 0, quarter), ag_recv.at[7])
    arrived(their_piece(dev + 2, quarter, quarter), ag_recv.at[8])

    @pl.loop(0, seqs // 16)
    def _(i):
        block = pl.ds(pl.multiple_of(i * 16, 16), 16)
        act[block, :] = rms(x1g[block, :], fgain[...])

    def gated(j, gate_w, up_w):
        gate = dot(act[...], gate_w)
        up = dot(act[...], up_w)
        here = u.at[core * n_col + j]
        here[...] = (jax.nn.silu(gate) * up).astype(BF16)
        send(here, here, u_send.at[j], u_recv.at[j], mate)

    @pl.loop(0, n_col - 1)
    def _(j):
        landed(wg.at[:, :, 0:COL], gu_sem.at[0, j])
        landed(wu.at[:, :, 0:COL], gu_sem.at[1, j])
        part = cols(j * COL, COL)
        gated(j, wg[:, :, part].reshape(prow * pcol, COL), wu[:, :, part].reshape(prow * pcol, COL))

    landed(kbuf.at[0:prow], gu_sem.at[0, n_col - 1])
    landed(vbuf.at[0:prow], gu_sem.at[1, n_col - 1])
    gated(n_col - 1, kbuf[0:prow].reshape(prow * pcol, COL), vbuf[0:prow].reshape(prow * pcol, COL))
    for j in range(n_col):
        arrived(u.at[(1 - core) * n_col + j], u_recv.at[j])

    def way(j):
        sign = (1 - 2 * core) * (1 - 2 * lax.rem(j, 2))
        return sign

    def rows_of(owner):
        return pl.ds(pl.multiple_of(lax.rem(owner + 2 * n_dev, n_dev) * rows, rows), rows)

    @pl.loop(0, n_col)
    def _(j):
        landed(wa.at[:, :, 0:COL], wd_sem.at[j])
        total_y = jnp.zeros((seqs, COL), F32)
        down = wa.at[:, :, cols(j * COL, COL)]
        full_u = jnp.concatenate([u[i] for i in range(2 * n_col)], axis=1)
        yb[j] = dot(full_u, down[...].reshape(prow * pcol, COL)) + total_y
        sign = way(j)
        send(yb.at[j, rows_of(dev + 2)], r1.at[j], rs_send.at[0, j], rs_recv.at[0, j], on_y(sign))
        send(yb.at[j, rows_of(dev - sign)], r3.at[j], rs_send.at[2, j], rs_recv.at[2, j], on_y(-sign))

    @pl.loop(0, n_col)
    def _(j):
        sign = way(j)
        arrived(r1.at[j], rs_recv.at[0, j])
        yb[j, rows_of(dev + sign), :] += r1[j]
        send(yb.at[j, rows_of(dev + sign)], r2.at[j], rs_send.at[1, j], rs_recv.at[1, j], on_y(sign))

    @pl.loop(0, n_col)
    def _(j):
        arrived(r2.at[j], rs_recv.at[1, j])
        arrived(r3.at[j], rs_recv.at[2, j])
        y = (yb[j, rows_of(dev), :] + r2[j] + r3[j]).astype(BF16)
        x1 = x1g[rows_of(dev), cols(core * half + j * COL, COL)]
        fin[:, cols(j * COL, COL)] = (x1.astype(F32) + y.astype(F32)).astype(BF16)

    blk = rows // CORES
    my_blk = pl.ds(pl.multiple_of(core * blk, blk), blk)
    mate_blk = pl.ds(pl.multiple_of((1 - core) * blk, blk), blk)
    send(fin.at[mate_blk], finr, fin_send.at[0], fin_recv.at[0], mate)
    store = pltpu.make_async_copy(fin.at[my_blk], out_hbm.at[:, mine], out_sem.at[0])
    store.start()
    arrived(finr, fin_recv.at[0])
    store2 = pltpu.make_async_copy(finr, out_hbm.at[:, other], out_sem.at[1])
    store2.start()

    for r in range(1, n_x):
        arrived(og.at[r], a2a_send.at[r])
    arrived(precv, pp_send.at[0])
    for i, ref in enumerate((own, own, below_a, above_b, own, below, above, far_a, far_b)):
        arrived(ref, ag_send.at[i])
    for j in range(n_col):
        arrived(u.at[0], u_send.at[j])
        for i in range(3):
            arrived(r1.at[0], rs_send.at[i, j])
    arrived(finr, fin_send.at[0])
    store.wait()
    store2.wait()


def solution(mesh):
    n_side = mesh.shape['side']
    n_dev = mesh.shape['dev']
    batch_axes = ('inst', 'dev')
    in_specs = (
        P(batch_axes, None),
        P(batch_axes),
        P(None, batch_axes, None, None, None),
        P(None, batch_axes, None, None, None),
        P(), P(), P(), P(), P(),
        P(None, None, 'dev'),
        P(None, None, 'dev'),
        P(None, 'dev', None),
    )
    out_specs = P(('inst', 'dev', 'side'), None)

    def device_fn(hidden, cache_len, k_cache, v_cache, w_q, w_kv, w_o, attn_gain, ffn_gain, w_gate, w_up, w_down):
        seqs, width = hidden.shape
        span, head = k_cache.shape[3:]
        ff = w_gate.shape[2]
        half = width // 2
        rows = seqs * CORES // n_side
        n_x = n_side // CORES
        n_col = half // COL
        q_cols = w_q.shape[2] // n_side
        tall = width // span
        freqs = jnp.asarray(ROPE_BASE ** (-np.arange(head // 2, dtype=np.float64) / (head // 2)), F32)[None]

        def fold(w):
            return w.reshape(w.shape[1] // span, span, w.shape[2])

        args = (hidden, cache_len.reshape(1, seqs), freqs, k_cache[0], v_cache[0], fold(w_q), fold(w_kv),
                w_o.reshape(n_side, w_o.shape[1] // n_side, width), attn_gain, ffn_gain,
                fold(w_gate), fold(w_up), fold(w_down))
        vmem = pltpu.VMEM
        dma = pltpu.SemaphoreType.DMA
        scratch = [
            vmem((seqs, width), BF16), vmem((1, seqs), jnp.int32), vmem((1, head // 2), F32),
            vmem((1, width), F32), vmem((1, width), F32), vmem((rows, half), BF16),
            vmem((tall, span, half), BF16),
            vmem((seqs, span, head), BF16), vmem((seqs, span, head), BF16),
            vmem((n_x, q_cols, width), BF16),
            vmem((tall, span, ff // 2 - COL), BF16), vmem((tall, span, ff // 2 - COL), BF16),
            vmem((n_col, seqs, COL), F32), vmem((2 * seqs, head), BF16),
            vmem((2 * seqs, 8 * span), F32), vmem((2 * seqs, 8 * span), BF16), vmem((2 * seqs, head), F32),
            vmem((seqs, q_cols), BF16), vmem((n_x, rows, q_cols), BF16),
            vmem((2 * n_col, rows, COL), F32), vmem((n_col, rows, COL), F32),
            vmem((n_dev * rows, width), BF16), vmem((2 * n_col, seqs, COL), BF16),
            vmem((n_col, rows, COL), F32), vmem((n_col, rows, COL), F32), vmem((n_col, rows, COL), F32),
            vmem((rows, half), BF16), vmem((rows // CORES, half), BF16),
            dma((6,)), dma((4,)), dma((2,)), dma((n_x,)), dma((2, n_col)), dma((n_col,)), dma((2,)),
            dma((n_x,)), dma((n_x,)), dma((1,)), dma((1,)), dma((9,)), dma((9,)), dma((n_col,)), dma((n_col,)),
            dma((3, n_col)), dma((3, n_col)), dma((1,)), dma((1,)),
        ]
        anywhere = pl.BlockSpec(memory_space=pl.ANY)
        return pl.pallas_call(
            functools.partial(layer_kernel, n_dev, n_side),
            out_shape=jax.ShapeDtypeStruct((rows // CORES, width), BF16),
            in_specs=[anywhere] * len(args),
            out_specs=anywhere,
            scratch_shapes=scratch,
            compiler_params=pltpu.CompilerParams(
                collective_id=0, has_side_effects=True, vmem_limit_bytes=67_043_328),
        )(*args)

    return jax.shard_map(device_fn, mesh=mesh, in_specs=in_specs, out_specs=out_specs, check_vma=False)
```

```python
import functools

import jax
import jax.numpy as jnp
import numpy as np
from jax import lax
from jax.experimental import pallas as pl
from jax.experimental.pallas import tpu as pltpu
from jax.sharding import PartitionSpec as P

EPS = 1e-5
ROPE_BASE = 10000.0
MESH = pl.DeviceIdType.MESH
F32 = jnp.float32
BF16 = jnp.bfloat16
COL = 256
CORES = 2
NEG = -1e30


def dot(lhs, rhs):
    return jnp.dot(lhs, rhs, preferred_element_type=F32)


def rms_scale(square_sum, width):
    return lax.rsqrt(square_sum / width + EPS)


def square_sums(parts):
    acc = None
    for part in parts:
        for g in range(part.shape[1] // 128):
            x = part[:, g * 128:(g + 1) * 128]
            acc = x * x if acc is None else acc + x * x
    return jnp.sum(acc, axis=1, keepdims=True)


def pair_blocks(first, second):
    rows, n = first.shape
    both = jnp.concatenate([first.reshape(rows // 8, 8, n), second.reshape(rows // 8, 8, n)], axis=1)
    return both.reshape(2 * rows, n)


class Phases:
    def __init__(self):
        self.scope = None

    def __call__(self, name):
        if self.scope is not None:
            self.scope.__exit__(None, None, None)
        self.scope = None if name is None else jax.named_scope(name)
        if self.scope is not None:
            self.scope.__enter__()


def layer_kernel(n_dev, n_side,
                 x_hbm, len_hbm, freq_hbm, k_hbm, v_hbm, wq_hbm, wkv_hbm, wo_hbm, again_hbm, fgain_hbm,
                 wg_hbm, wu_hbm, wd_hbm, out_hbm,
                 act, lens, freqs, again, fgain, xres, wa, kbuf, vbuf, wo, wg, wu,
                 yb, ub, qa, sb, pb, ob, osend, og, pp, precv, x1b, hg, u, r1, r2, r3, fin,
                 in_sem, w_sem, kv_sem, wo_sem, gu_sem, tail_sem, wd_sem, out_sem,
                 a2a_send, a2a_recv, pp_send, pp_recv, ag_send, ag_recv, u_send, u_recv,
                 rs_send, rs_recv, fin_send, fin_recv):
    dev = lax.axis_index('dev')
    side = lax.axis_index('side')
    n_x = n_side // CORES
    chip = lax.div(side, CORES)
    core = lax.rem(side, CORES)
    mate = {'side': CORES * chip + 1 - core}
    seqs, width = act.shape
    head = COL
    q_cols = osend.shape[1]
    half = width // 2
    rows = xres.shape[0]
    n_col = half // COL
    kq = (n_col + 1) // 2 * COL // wa.shape[1]
    n_main = wg.shape[2] // COL
    n_tail = n_col - n_main
    kv_half = wkv_hbm.shape[2] // 2
    prow, pcol = wa.shape[0], wa.shape[1]

    def on_x(r):
        return {'side': CORES * lax.rem(chip + r, n_x) + core}

    def on_y(r):
        return {'dev': lax.rem(dev + r + n_dev, n_dev)}

    phase = Phases()
    phase('start')
    barrier = pltpu.get_barrier_semaphore()
    peers = [mate] + [on_x(r) for r in range(1, n_x)] + [on_y(1), on_y(-1)]
    for peer in peers:
        pl.semaphore_signal(barrier, inc=1, device_id=peer, device_id_type=MESH)

    def cols(start, size):
        return pl.ds(pl.multiple_of(start, 128), size)

    def load(src, dst, sem, priority=1):
        pltpu.make_async_copy(src, dst, sem).start(priority=priority)

    def landed(dst, sem):
        pltpu.make_async_copy(dst, dst, sem).wait()

    mine = cols(core * half, half)
    other = cols((1 - core) * half, half)
    my_rows = pl.ds(pl.multiple_of(chip * rows, rows), rows)

    load(x_hbm, act, in_sem.at[0], 0)
    load(len_hbm, lens, in_sem.at[1], 0)
    load(freq_hbm, freqs, in_sem.at[2], 0)
    load(again_hbm, again, in_sem.at[3], 0)
    load(fgain_hbm, fgain, in_sem.at[4], 0)
    load(x_hbm.at[my_rows], xres, in_sem.at[5], 0)

    def w_slot(j):
        return wa.at[:, :, j * COL:(j + 1) * COL]

    load(wq_hbm.at[:, :, cols(side * q_cols, COL)], w_slot(0), w_sem.at[0], 0)
    load(wq_hbm.at[:, :, cols(side * q_cols + COL, COL)], w_slot(1), w_sem.at[1], 0)
    load(wkv_hbm.at[:, :, cols(side * head, COL)], w_slot(2), w_sem.at[2], 0)
    load(wkv_hbm.at[:, :, cols(kv_half + side * head, COL)], w_slot(3), w_sem.at[3], 0)
    phase('wait_x')
    for i, ref in enumerate((act, lens, freqs, again, fgain, xres)):
        landed(ref, in_sem.at[i])
    load(k_hbm.at[:, side], kbuf, kv_sem.at[0], 0)
    load(v_hbm.at[:, side], vbuf, kv_sem.at[1], 0)
    for r in range(n_x):
        src_chip = lax.rem(chip + n_x - r, n_x)
        load(wo_hbm.at[CORES * src_chip + core], wo.at[r], wo_sem.at[r])
    phase('tables')
    row_id = lax.broadcasted_iota(jnp.int32, (seqs, seqs), 0)
    col_id = lax.broadcasted_iota(jnp.int32, (seqs, seqs), 1)
    wide = jnp.broadcast_to(lens[...].astype(F32), (seqs, seqs))
    len_col = jnp.sum(jnp.where(row_id == col_id, wide, 0.0), axis=1, keepdims=True)
    angle = len_col * freqs[...]
    cos_part = jnp.cos(angle)
    sin_part = jnp.sin(angle)

    def rotate(vecs):
        first, second = vecs[:, :head // 2], vecs[:, head // 2:]
        return jnp.concatenate([first * cos_part - second * sin_part, second * cos_part + first * sin_part], axis=1)

    phase('norm1')
    inv = rms_scale(square_sums([act[:, i * COL:(i + 1) * COL].astype(F32) for i in range(2 * n_col)]), width)
    for i in range(2 * n_col):
        part = slice(i * COL, (i + 1) * COL)
        act[:, part] = (act[:, part].astype(F32) * inv * again[:, part]).astype(BF16)

    phase('qkv')
    @pl.loop(0, 4)
    def _(j):
        landed(w_slot(0), w_sem.at[j])
        w = wa[:, :, cols(j * COL, COL)].reshape(prow * pcol, COL)
        yb[j] = dot(act[...], w)

    phase('rope')
    q0 = rotate(yb[0]).astype(BF16).astype(F32)
    q1 = rotate(yb[1]).astype(BF16).astype(F32)
    k_new = rotate(yb[2]).astype(BF16).astype(F32)
    v_new = yb[3].astype(BF16).astype(F32)
    qa[...] = pair_blocks(q0, q1).astype(BF16)
    scale = head ** -0.5
    self0 = jnp.sum(q0 * k_new, axis=1, keepdims=True)
    self1 = jnp.sum(q1 * k_new, axis=1, keepdims=True)
    self_score = pair_blocks(self0, self1) * scale
    len_rows = pair_blocks(len_col, len_col).astype(jnp.int32)

    span = kbuf.shape[1]
    keys = 8 * span
    phase('wait_k')
    landed(kbuf, kv_sem.at[0])
    phase('scores')
    for b in range(seqs // 8):
        k_blk = kbuf[8 * b:8 * b + 8].reshape(keys, head)
        sb[16 * b:16 * b + 16, :] = lax.dot_general(
            qa[16 * b:16 * b + 16, :], k_blk, (((1,), (1,)), ((), ())), preferred_element_type=F32)
    phase('softmax')
    row = lax.broadcasted_iota(jnp.int32, (2 * seqs, keys), 0)
    key = lax.broadcasted_iota(jnp.int32, (2 * seqs, keys), 1)
    offset = key - lax.rem(row, 8) * span
    valid = (offset >= 0) & (offset < len_rows)
    scores = jnp.where(valid, sb[...] * scale, NEG)
    row_max = jnp.maximum(jnp.max(scores, axis=1, keepdims=True), self_score)
    exp_scores = jnp.exp(scores - row_max)
    self_exp = jnp.exp(self_score - row_max)
    total = jnp.sum(exp_scores, axis=1, keepdims=True) + self_exp
    pb[...] = exp_scores.astype(BF16)
    phase('wait_v')
    landed(vbuf, kv_sem.at[1])
    phase('mix')
    for b in range(seqs // 8):
        v_blk = vbuf[8 * b:8 * b + 8].reshape(keys, head)
        ob[16 * b:16 * b + 16, :] = dot(pb[16 * b:16 * b + 16, :], v_blk)
    mixed = ob[...] + self_exp.astype(BF16).astype(F32) * pair_blocks(v_new, v_new)
    mixed = (mixed / total).reshape(seqs // 8, 16, head)
    osend[:, :head] = mixed[:, :8].reshape(seqs, head).astype(BF16)
    osend[:, head:] = mixed[:, 8:].reshape(seqs, head).astype(BF16)

    phase('loads2')
    seg = ((0, kq), (half // pcol, kq), (kq, half // pcol - kq), (half // pcol + kq, half // pcol - kq))

    def load_gate_up(part):
        for i in (2 * part, 2 * part + 1):
            first, count = seg[i]
            at = pl.ds(first, count)
            for m, (w_hbm, w_buf, tail) in enumerate(((wg_hbm, wg, kbuf), (wu_hbm, wu, vbuf))):
                load(w_hbm.at[at, :, cols(core * half, n_main * COL)], w_buf.at[at], gu_sem.at[m, i])
                for t in range(n_tail):
                    load(w_hbm.at[at, :, cols(core * half + (n_main + t) * COL, COL)],
                         tail.at[pl.ds(t * prow + first, count)], tail_sem.at[m, t, i])

    load_gate_up(0)
    load_gate_up(1)
    phase('a2a_start')
    pl.semaphore_wait(barrier, len(peers))

    def send(src, dst, send_sem, recv_sem, where):
        pltpu.make_async_remote_copy(src, dst, send_sem, recv_sem, device_id=where, device_id_type=MESH).start()

    def arrived(dst, sem):
        pltpu.make_async_copy(dst, dst, sem).wait()

    for r in range(1, n_x):
        there = lax.rem(chip + r, n_x)
        send(osend.at[pl.ds(pl.multiple_of(there * rows, rows), rows)], og.at[r], a2a_send.at[r], a2a_recv.at[r], on_x(r))

    phase('proj')
    steps = [0, 1] + [r for r in range(n_x - 1, 1, -1)]
    for r in steps[:-1]:
        landed(wo.at[r], wo_sem.at[r])
        if r == 0:
            pp[...] = dot(osend[my_rows, :], wo[0])
        else:
            arrived(og.at[r], a2a_recv.at[r])
            pp[...] += dot(og[r], wo[r])
    r = steps[-1]
    landed(wo.at[r], wo_sem.at[r])
    arrived(og.at[r], a2a_recv.at[r])
    for i in range(2):
        part = slice(i * half, (i + 1) * half)
        pp[:, part] += dot(og[r], wo[r, :, part])
        send(pp.at[:, part], precv.at[:, part], pp_send.at[i], pp_recv.at[i], mate)
    for j in range(n_col):
        load(wd_hbm.at[:, :, cols(core * half + j * COL, COL)], wa.at[:, :, j * COL:(j + 1) * COL], wd_sem.at[j])

    phase('wait_mate')
    dev_rows = pl.ds(pl.multiple_of(dev * rows, rows), rows)
    for i in range(2):
        part = slice(i * half, (i + 1) * half)
        arrived(precv.at[:, part], pp_recv.at[i])
        x1b[:, part] = (xres[:, part].astype(F32) + (pp[:, part] + precv[:, part])).astype(BF16)
    phase('norm2')
    inv2 = rms_scale(square_sums([x1b[:, i * COL:(i + 1) * COL].astype(F32) for i in range(2 * n_col)]), width)
    for i in range(2 * n_col):
        part = slice(i * COL, (i + 1) * COL)
        hg[dev_rows, part] = (x1b[:, part].astype(F32) * inv2 * fgain[:, part]).astype(BF16)

    phase('gather')
    ka = kq * pcol // 2
    kb = (half - kq * pcol) // 2
    strips = (((0, ka), (ka, ka)), ((2 * ka, kb), (2 * ka + kb, kb)))

    def piece(owner, strip, whose):
        owner_rows = pl.ds(pl.multiple_of(lax.rem(owner + 2 * n_dev, n_dev) * rows, rows), rows)
        return hg.at[owner_rows, cols(whose * half + strip[0], strip[1])]

    def hop(owner, strip, p, i, where):
        ref = piece(owner, strip, core)
        send(ref, ref, ag_send.at[p, i], ag_recv.at[p, i], where)

    def came(owner, strip, p, i):
        arrived(piece(owner, strip, core), ag_recv.at[p, i])

    source = ((-1, 0), (1, 1), (-1, 1), (1, 0), (2, 0), (2, 1))
    for p in range(2):
        hop(dev, strips[p][0], p, 0, on_y(1))
        hop(dev, strips[p][1], p, 1, on_y(-1))
        hop(dev, strips[p][1], p, 2, on_y(1))
        hop(dev, strips[p][0], p, 3, on_y(-1))

    def take(p, i):
        owner, strip = dev + source[i][0], strips[p][source[i][1]]
        came(owner, strip, p, i)
        if i < 2:
            hop(owner, strip, p, 4 + i, on_y(1 - 2 * i))
        hop(owner, strip, p, 6 + i, mate)

    def from_mate(p):
        for i in range(6):
            owner, strip = dev + source[i][0], strips[p][source[i][1]]
            arrived(piece(owner, strip, 1 - core), ag_recv.at[p, 6 + i])

    def weights(m, j, i):
        first, count = seg[i]
        main, tail = (wg, kbuf) if m == 0 else (wu, vbuf)
        if isinstance(j, int) and j >= n_main:
            start = (j - n_main) * prow + first
            return tail[start:start + count].reshape(count * pcol, COL)
        return main[first:first + count, :, cols(j * COL, COL)].reshape(count * pcol, COL)

    def partial_sum(m, j, p):
        out = None
        for i in (2 * p, 2 * p + 1):
            first, count = seg[i]
            term = dot(hg[:, first * pcol:(first + count) * pcol], weights(m, j, i))
            out = term if out is None else out + term
        return out

    def gate_up(p, j):
        gate, up = partial_sum(0, j, p), partial_sum(1, j, p)
        if p == 0:
            yb[j] = gate
            ub[j] = up
        else:
            here = u.at[core * n_col + j]
            here[...] = (jax.nn.silu(yb[j] + gate) * (ub[j] + up)).astype(BF16)
            send(here, here, u_send.at[j], u_recv.at[j], mate)

    def gate_up_part(p):
        for i in (2 * p, 2 * p + 1):
            first, count = seg[i]
            for m, (w_buf, tail) in enumerate(((wg, kbuf), (wu, vbuf))):
                landed(w_buf.at[pl.ds(first, count)], gu_sem.at[m, i])
                for t in range(n_tail):
                    landed(tail.at[pl.ds(t * prow + first, count)], tail_sem.at[m, t, i])
        phase('gateup%d' % p)

        @pl.loop(0, n_main)
        def _(j):
            gate_up(p, j)

        for t in range(n_tail):
            gate_up(p, n_main + t)

    for p, i in ((0, 0), (0, 1), (0, 2), (0, 3), (1, 0), (1, 1), (0, 4), (0, 5), (1, 2), (1, 3)):
        take(p, i)
    from_mate(0)
    phase('wait_gu0')
    gate_up_part(0)
    phase('gather2')
    take(1, 4)
    take(1, 5)
    from_mate(1)
    phase('wait_gu1')
    gate_up_part(1)
    phase('down0')
    ahead = 3
    fold_half = half // pcol

    def u_half(whose):
        return jnp.concatenate([u[whose * n_col + i] for i in range(n_col)], axis=1)

    def down_half(whose, j):
        at = pl.ds(whose * fold_half, fold_half)
        return dot(u_half(whose), wa[at, :, cols(j * COL, COL)].reshape(half, COL))

    @pl.loop(0, ahead)
    def _(j):
        landed(wa.at[:, :, 0:COL], wd_sem.at[j])
        yb[j] = down_half(core, j)

    phase('wait_u')
    for j in range(n_col):
        arrived(u.at[(1 - core) * n_col + j], u_recv.at[j])

    phase('down')
    def way(j):
        sign = (1 - 2 * core) * (1 - 2 * lax.rem(j, 2))
        return sign

    def rows_of(owner):
        return pl.ds(pl.multiple_of(lax.rem(owner + 2 * n_dev, n_dev) * rows, rows), rows)

    def pass_on(j):
        sign = way(j)
        send(yb.at[j, rows_of(dev + 2)], r1.at[j], rs_send.at[0, j], rs_recv.at[0, j], on_y(sign))
        send(yb.at[j, rows_of(dev - sign)], r3.at[j], rs_send.at[2, j], rs_recv.at[2, j], on_y(-sign))

    @pl.loop(0, ahead)
    def _(j):
        yb[j] += down_half(1 - core, j)
        pass_on(j)

    @pl.loop(ahead, n_col)
    def _(j):
        landed(wa.at[:, :, 0:COL], wd_sem.at[j])
        yb[j] = dot(jnp.concatenate([u[i] for i in range(2 * n_col)], axis=1),
                    wa[:, :, cols(j * COL, COL)].reshape(prow * pcol, COL))
        pass_on(j)

    phase('stage2')
    @pl.loop(0, n_col)
    def _(j):
        sign = way(j)
        arrived(r1.at[j], rs_recv.at[0, j])
        yb[j, rows_of(dev + sign), :] += r1[j]
        send(yb.at[j, rows_of(dev + sign)], r2.at[j], rs_send.at[1, j], rs_recv.at[1, j], on_y(sign))

    phase('final')
    @pl.loop(0, n_col)
    def _(j):
        arrived(r2.at[j], rs_recv.at[1, j])
        arrived(r3.at[j], rs_recv.at[2, j])
        y = (yb[j, rows_of(dev), :] + r2[j] + r3[j]).astype(BF16)
        x1 = x1b[:, cols(core * half + j * COL, COL)]
        fin[:, cols(j * COL, COL)] = (x1.astype(F32) + y.astype(F32)).astype(BF16)

    phase('fin')
    blk = rows // CORES
    my_blk = pl.ds(pl.multiple_of(core * blk, blk), blk)
    mate_blk = pl.ds(pl.multiple_of((1 - core) * blk, blk), blk)
    send(fin.at[mate_blk], out_hbm.at[:, mine], fin_send.at[0], fin_recv.at[0], mate)
    store = pltpu.make_async_copy(fin.at[my_blk], out_hbm.at[:, mine], out_sem.at[0])
    store.start()
    arrived(out_hbm.at[:, other], fin_recv.at[0])
    phase('drain')
    for r in range(1, n_x):
        arrived(og.at[r], a2a_send.at[r])
    for i in range(2):
        part = slice(i * half, (i + 1) * half)
        arrived(precv.at[:, part], pp_send.at[i])
    for p in range(2):
        for i in range(12):
            strip = strips[p][(0, 1, 1, 0, 0, 1, 0, 1, 1, 0, 0, 1)[i]]
            arrived(piece(dev, strip, core), ag_send.at[p, i])
    for j in range(n_col):
        arrived(u.at[0], u_send.at[j])
        for i in range(3):
            arrived(r1.at[0], rs_send.at[i, j])
    arrived(fin.at[mate_blk], fin_send.at[0])
    store.wait()
    phase(None)


def solution(mesh):
    n_side = mesh.shape['side']
    n_dev = mesh.shape['dev']
    batch_axes = ('inst', 'dev')
    in_specs = (
        P(batch_axes, None),
        P(batch_axes),
        P(None, batch_axes, None, None, None),
        P(None, batch_axes, None, None, None),
        P(), P(), P(), P(), P(),
        P(None, None, 'dev'),
        P(None, None, 'dev'),
        P(None, 'dev', None),
    )
    out_specs = P(('inst', 'dev', 'side'), None)

    def device_fn(hidden, cache_len, k_cache, v_cache, w_q, w_kv, w_o, attn_gain, ffn_gain, w_gate, w_up, w_down):
        seqs, width = hidden.shape
        span, head = k_cache.shape[3:]
        ff = w_gate.shape[2]
        half = width // 2
        rows = seqs * CORES // n_side
        n_x = n_side // CORES
        n_col = half // COL
        q_cols = w_q.shape[2] // n_side
        tall = width // span
        freqs = jnp.asarray(ROPE_BASE ** (-np.arange(head // 2, dtype=np.float64) / (head // 2)), F32)[None]

        def fold(w):
            return w.reshape(w.shape[1] // span, span, w.shape[2])

        args = (hidden, cache_len.reshape(1, seqs), freqs, k_cache[0], v_cache[0], fold(w_q), fold(w_kv),
                w_o.reshape(n_side, w_o.shape[1] // n_side, width), attn_gain, ffn_gain,
                fold(w_gate), fold(w_up), fold(w_down))
        vmem = pltpu.VMEM
        dma = pltpu.SemaphoreType.DMA
        main = ff // CORES - 2 * COL
        scratch = [
            vmem((seqs, width), BF16), vmem((1, seqs), jnp.int32), vmem((1, head // 2), F32),
            vmem((1, width), F32), vmem((1, width), F32), vmem((rows, width), BF16),
            vmem((tall, span, half), BF16),
            vmem((seqs, span, head), BF16), vmem((seqs, span, head), BF16),
            vmem((n_x, q_cols, width), BF16),
            vmem((tall, span, main), BF16), vmem((tall, span, main), BF16),
            vmem((n_col, seqs, COL), F32), vmem((n_col, seqs, COL), F32), vmem((2 * seqs, head), BF16),
            vmem((2 * seqs, 8 * span), F32), vmem((2 * seqs, 8 * span), BF16), vmem((2 * seqs, head), F32),
            vmem((seqs, q_cols), BF16), vmem((n_x, rows, q_cols), BF16),
            vmem((rows, width), F32), vmem((rows, width), F32), vmem((rows, width), BF16),
            vmem((n_dev * rows, width), BF16), vmem((2 * n_col, seqs, COL), BF16),
            vmem((n_col, rows, COL), F32), vmem((n_col, rows, COL), F32), vmem((n_col, rows, COL), F32),
            vmem((rows, half), BF16),
            dma((6,)), dma((4,)), dma((2,)), dma((n_x,)), dma((2, 4)), dma((2, 2, 4)), dma((n_col,)), dma((1,)),
            dma((n_x,)), dma((n_x,)), dma((2,)), dma((2,)), dma((2, 12)), dma((2, 12)), dma((n_col,)), dma((n_col,)),
            dma((3, n_col)), dma((3, n_col)), dma((1,)), dma((1,)),
        ]
        anywhere = pl.BlockSpec(memory_space=pl.ANY)
        return pl.pallas_call(
            functools.partial(layer_kernel, n_dev, n_side),
            out_shape=jax.ShapeDtypeStruct((rows // CORES, width), BF16),
            in_specs=[anywhere] * len(args),
            out_specs=anywhere,
            scratch_shapes=scratch,
            compiler_params=pltpu.CompilerParams(
                collective_id=0, has_side_effects=True, vmem_limit_bytes=67_043_328),
        )(*args)

    return jax.shard_map(device_fn, mesh=mesh, in_specs=in_specs, out_specs=out_specs, check_vma=False)
```

```python
import functools

import jax
import jax.numpy as jnp
import numpy as np
from jax import lax
from jax.experimental import pallas as pl
from jax.experimental.pallas import tpu as pltpu
from jax.sharding import PartitionSpec as P

EPS = 1e-5
ROPE_BASE = 10000.0
MESH = pl.DeviceIdType.MESH
F32 = jnp.float32
BF16 = jnp.bfloat16
COL = 256
CORES = 2
NEG = -1e30


def dot(lhs, rhs):
    return jnp.dot(lhs, rhs, preferred_element_type=F32)


def rms_scale(square_sum, width):
    return lax.rsqrt(square_sum / width + EPS)


def square_sums(parts):
    acc = None
    for part in parts:
        for g in range(part.shape[1] // 128):
            x = part[:, g * 128:(g + 1) * 128]
            acc = x * x if acc is None else acc + x * x
    return jnp.sum(acc, axis=1, keepdims=True)


def pair_blocks(first, second):
    rows, n = first.shape
    both = jnp.concatenate([first.reshape(rows // 8, 8, n), second.reshape(rows // 8, 8, n)], axis=1)
    return both.reshape(2 * rows, n)


class Phases:
    def __init__(self):
        self.scope = None

    def __call__(self, name):
        if self.scope is not None:
            self.scope.__exit__(None, None, None)
        self.scope = None if name is None else jax.named_scope(name)
        if self.scope is not None:
            self.scope.__enter__()


def layer_kernel(n_dev, n_side,
                 x_hbm, len_hbm, freq_hbm, k_hbm, v_hbm, wq_hbm, wkv_hbm, wo_hbm, again_hbm, fgain_hbm,
                 wg_hbm, wu_hbm, wd_hbm, out_hbm,
                 act, lens, freqs, again, fgain, xres, wa, kbuf, vbuf, wo, wg, wu,
                 yb, ub, lenc, osend, og, pp, precv, x1b, hg, u, r1, r2, r3, fin,
                 in_sem, w_sem, kv_sem, wo_sem, gu_sem, tail_sem, wd_sem, out_sem,
                 a2a_send, a2a_recv, pp_send, pp_recv, ag_send, ag_recv, u_send, u_recv,
                 rs_send, rs_recv, fin_send, fin_recv):
    dev = lax.axis_index('dev')
    side = lax.axis_index('side')
    n_x = n_side // CORES
    chip = lax.div(side, CORES)
    core = lax.rem(side, CORES)
    mate = {'side': CORES * chip + 1 - core}
    seqs, width = act.shape
    head = COL
    q_cols = osend.shape[1]
    half = width // 2
    rows = xres.shape[0]
    n_col = half // COL
    kq = (n_col + 1) // 2 * COL // wa.shape[1]
    n_main = wg.shape[2] // COL
    n_tail = n_col - n_main
    kv_half = wkv_hbm.shape[2] // 2
    prow, pcol = wa.shape[0], wa.shape[1]

    def on_x(r):
        return {'side': CORES * lax.rem(chip + r, n_x) + core}

    def on_y(r):
        return {'dev': lax.rem(dev + r + n_dev, n_dev)}

    phase = Phases()
    phase('start')
    barrier = pltpu.get_barrier_semaphore()
    peers = [mate] + [on_x(r) for r in range(1, n_x)] + [on_y(1), on_y(-1)]
    for peer in peers:
        pl.semaphore_signal(barrier, inc=1, device_id=peer, device_id_type=MESH)

    def cols(start, size):
        return pl.ds(pl.multiple_of(start, 128), size)

    def load(src, dst, sem, priority=1):
        pltpu.make_async_copy(src, dst, sem).start(priority=priority)

    def landed(dst, sem):
        pltpu.make_async_copy(dst, dst, sem).wait()

    mine = cols(core * half, half)
    other = cols((1 - core) * half, half)
    my_rows = pl.ds(pl.multiple_of(chip * rows, rows), rows)

    load(x_hbm, act, in_sem.at[0], 0)
    load(len_hbm, lens, in_sem.at[1], 0)
    load(freq_hbm, freqs, in_sem.at[2], 0)
    load(again_hbm, again, in_sem.at[3], 0)
    load(fgain_hbm, fgain, in_sem.at[4], 0)
    load(x_hbm.at[my_rows], xres, in_sem.at[5], 0)

    def w_slot(j):
        return wa.at[:, :, j * COL:(j + 1) * COL]

    load(wq_hbm.at[:, :, cols(side * q_cols, COL)], w_slot(0), w_sem.at[0])
    load(wq_hbm.at[:, :, cols(side * q_cols + COL, COL)], w_slot(1), w_sem.at[1])
    load(wkv_hbm.at[:, :, cols(side * head, COL)], w_slot(2), w_sem.at[2])
    load(wkv_hbm.at[:, :, cols(kv_half + side * head, COL)], w_slot(3), w_sem.at[3])
    phase('wait_x')
    for i, ref in enumerate((act, lens, freqs, again, fgain, xres)):
        landed(ref, in_sem.at[i])
    by_distance = sorted(range(1, n_x), key=lambda r: (-min(r, n_x - r), -r)) + [0]

    def cache_rows(r):
        return pl.ds(lax.rem(chip + r, n_x) * rows, rows)

    def load_cache(r):
        at = cache_rows(r)
        load(k_hbm.at[at, side], kbuf.at[at], kv_sem.at[0, r])
        load(v_hbm.at[at, side], vbuf.at[at], kv_sem.at[1, r])

    def load_wo(r):
        src_chip = lax.rem(chip + n_x - r, n_x)
        load(wo_hbm.at[CORES * src_chip + core], wo.at[r], wo_sem.at[r])

    load_cache(by_distance[0])
    phase('tables')
    row_id = lax.broadcasted_iota(jnp.int32, (seqs, seqs), 0)
    col_id = lax.broadcasted_iota(jnp.int32, (seqs, seqs), 1)
    wide = jnp.broadcast_to(lens[...].astype(F32), (seqs, seqs))
    len_col = jnp.sum(jnp.where(row_id == col_id, wide, 0.0), axis=1, keepdims=True)
    angle = len_col * freqs[...]
    cos_part = jnp.cos(angle)
    sin_part = jnp.sin(angle)

    def rotate(vecs):
        first, second = vecs[:, :head // 2], vecs[:, head // 2:]
        return jnp.concatenate([first * cos_part - second * sin_part, second * cos_part + first * sin_part], axis=1)

    phase('norm1')
    inv = rms_scale(square_sums([act[:, i * COL:(i + 1) * COL].astype(F32) for i in range(2 * n_col)]), width)
    for i in range(2 * n_col):
        part = slice(i * COL, (i + 1) * COL)
        act[:, part] = (act[:, part].astype(F32) * inv * again[:, part]).astype(BF16)

    phase('qkv')
    lenc[...] = len_col

    for j in range(4):
        landed(w_slot(0), w_sem.at[j])
        if j + 1 < n_x:
            load_cache(by_distance[j + 1])
        yb[j] = dot(act[...], wa[:, :, cols(j * COL, COL)].reshape(prow * pcol, COL))

    load_wo(0)
    load_wo(by_distance[1])
    phase('rope')
    for j in range(4):
        vecs = yb[j] if j == 3 else rotate(yb[j])
        yb[j] = vecs.astype(BF16).astype(F32)

    span = kbuf.shape[1]
    keys = 8 * span
    scale = head ** -0.5
    groups = rows // 8
    row = lax.broadcasted_iota(jnp.int32, (2 * rows, keys), 0)
    key = lax.broadcasted_iota(jnp.int32, (2 * rows, keys), 1)
    offset = key - lax.rem(row, 8) * span

    def cat(parts):
        return parts[0] if len(parts) == 1 else jnp.concatenate(parts, axis=0)

    def attend(theres):
        ats = [pl.ds(pl.multiple_of(there * rows, rows), rows) for there in theres]
        q0, q1, k_new, v_new = (cat([yb[j, at, :] for at in ats]) for j in range(4))
        q_pair = pair_blocks(q0, q1).astype(BF16)
        self_score = pair_blocks(jnp.sum(q0 * k_new, axis=1, keepdims=True),
                                 jnp.sum(q1 * k_new, axis=1, keepdims=True)) * scale
        lengths = cat([lenc[at, :] for at in ats])
        len_rows = pair_blocks(lengths, lengths).astype(jnp.int32)
        blocks = [there * rows + 8 * b for there in theres for b in range(groups)]
        scores = cat([
            lax.dot_general(q_pair[16 * n:16 * n + 16], kbuf[pl.ds(b, 8)].reshape(keys, head),
                            (((1,), (1,)), ((), ())), preferred_element_type=F32)
            for n, b in enumerate(blocks)])
        offsets = cat([offset] * len(theres))
        scores = jnp.where((offsets >= 0) & (offsets < len_rows), scores * scale, NEG)
        row_max = jnp.maximum(jnp.max(scores, axis=1, keepdims=True), self_score)
        exp_scores = jnp.exp(scores - row_max)
        self_exp = jnp.exp(self_score - row_max)
        total = jnp.sum(exp_scores, axis=1, keepdims=True) + self_exp
        probs = exp_scores.astype(BF16)
        mixed = cat([dot(probs[16 * n:16 * n + 16], vbuf[pl.ds(b, 8)].reshape(keys, head))
                     for n, b in enumerate(blocks)])
        mixed = mixed + self_exp.astype(BF16).astype(F32) * pair_blocks(v_new, v_new)
        mixed = (mixed / total).reshape(len(blocks), 16, head)
        first = mixed[:, :8].reshape(len(theres) * rows, head).astype(BF16)
        second = mixed[:, 8:].reshape(len(theres) * rows, head).astype(BF16)
        for n, at in enumerate(ats):
            osend[at, :head] = first[n * rows:(n + 1) * rows]
            osend[at, head:] = second[n * rows:(n + 1) * rows]
        return ats

    def send(src, dst, send_sem, recv_sem, where):
        pltpu.make_async_remote_copy(src, dst, send_sem, recv_sem, device_id=where, device_id_type=MESH).start()

    def arrived(dst, sem):
        pltpu.make_async_copy(dst, dst, sem).wait()

    pl.semaphore_wait(barrier, len(peers))
    for pair in (by_distance[:2], by_distance[2:]):
        phase('wait_kv%d' % pair[0])
        for r in pair:
            landed(kbuf.at[cache_rows(r)], kv_sem.at[0, r])
            landed(vbuf.at[cache_rows(r)], kv_sem.at[1, r])
        phase('attend%d' % pair[0])
        ats = attend([lax.rem(chip + r, n_x) for r in pair])
        for r, at in zip(pair, ats):
            if r:
                send(osend.at[at], og.at[r], a2a_send.at[r], a2a_recv.at[r], on_x(r))
        if pair[0] == by_distance[0]:
            load_wo(by_distance[0])
            load_wo(by_distance[2])

    phase('loads2')
    seg = ((0, kq), (half // pcol, kq), (kq, half // pcol - kq), (half // pcol + kq, half // pcol - kq))

    def load_gate_up(part):
        for i in (2 * part, 2 * part + 1):
            first, count = seg[i]
            at = pl.ds(first, count)
            for m, (w_hbm, w_buf, tail) in enumerate(((wg_hbm, wg, kbuf), (wu_hbm, wu, vbuf))):
                load(w_hbm.at[at, :, cols(core * half, n_main * COL)], w_buf.at[at], gu_sem.at[m, i])
                for t in range(n_tail):
                    load(w_hbm.at[at, :, cols(core * half + (n_main + t) * COL, COL)],
                         tail.at[pl.ds(t * prow + first, count)], tail_sem.at[m, t, i])

    load_gate_up(0)
    load_gate_up(1)
    phase('proj')
    steps = [0] + by_distance[1:-1] + by_distance[:1]
    for r in steps[:-1]:
        phase('proj%d' % r)
        landed(wo.at[r], wo_sem.at[r])
        if r == 0:
            pp[...] = dot(osend[my_rows, :], wo[0])
        else:
            arrived(og.at[r], a2a_recv.at[r])
            pp[...] += dot(og[r], wo[r])
    r = steps[-1]
    phase('proj%d' % r)
    landed(wo.at[r], wo_sem.at[r])
    arrived(og.at[r], a2a_recv.at[r])
    for i in range(2):
        part = slice(i * half, (i + 1) * half)
        pp[:, part] += dot(og[r], wo[r, :, part])
        send(pp.at[:, part], precv.at[:, part], pp_send.at[i], pp_recv.at[i], mate)
    for j in range(n_col):
        load(wd_hbm.at[:, :, cols(core * half + j * COL, COL)], wa.at[:, :, j * COL:(j + 1) * COL], wd_sem.at[j])

    phase('wait_mate')
    dev_rows = pl.ds(pl.multiple_of(dev * rows, rows), rows)
    for i in range(2):
        part = slice(i * half, (i + 1) * half)
        arrived(precv.at[:, part], pp_recv.at[i])
        x1b[:, part] = (xres[:, part].astype(F32) + (pp[:, part] + precv[:, part])).astype(BF16)
    phase('norm2')
    inv2 = rms_scale(square_sums([x1b[:, i * COL:(i + 1) * COL].astype(F32) for i in range(2 * n_col)]), width)
    for i in range(2 * n_col):
        part = slice(i * COL, (i + 1) * COL)
        hg[dev_rows, part] = (x1b[:, part].astype(F32) * inv2 * fgain[:, part]).astype(BF16)

    phase('gather')
    ka = kq * pcol // 2
    kb = (half - kq * pcol) // 2
    strips = (((0, ka), (ka, ka)), ((2 * ka, kb), (2 * ka + kb, kb)))

    def piece(owner, strip, whose):
        owner_rows = pl.ds(pl.multiple_of(lax.rem(owner + 2 * n_dev, n_dev) * rows, rows), rows)
        return hg.at[owner_rows, cols(whose * half + strip[0], strip[1])]

    def hop(owner, strip, p, i, where):
        ref = piece(owner, strip, core)
        send(ref, ref, ag_send.at[p, i], ag_recv.at[p, i], where)

    def came(owner, strip, p, i):
        arrived(piece(owner, strip, core), ag_recv.at[p, i])

    source = ((-1, 0), (1, 1), (-1, 1), (1, 0), (2, 0), (2, 1))
    def hop_own(p, late):
        if late:
            hop(dev, strips[p][1], p, 2, on_y(1))
            hop(dev, strips[p][0], p, 3, on_y(-1))
        else:
            hop(dev, strips[p][0], p, 0, on_y(1))
            hop(dev, strips[p][1], p, 1, on_y(-1))

    hop_own(0, False)
    hop_own(0, True)
    hop_own(1, False)

    def take(p, i):
        owner, strip = dev + source[i][0], strips[p][source[i][1]]
        came(owner, strip, p, i)
        if i < 2:
            hop(owner, strip, p, 4 + i, on_y(1 - 2 * i))
        hop(owner, strip, p, 6 + i, mate)

    def from_mate(p):
        for i in range(6):
            owner, strip = dev + source[i][0], strips[p][source[i][1]]
            arrived(piece(owner, strip, 1 - core), ag_recv.at[p, 6 + i])

    def weights(m, j, i):
        first, count = seg[i]
        main, tail = (wg, kbuf) if m == 0 else (wu, vbuf)
        if isinstance(j, int) and j >= n_main:
            start = (j - n_main) * prow + first
            return tail[start:start + count].reshape(count * pcol, COL)
        return main[first:first + count, :, cols(j * COL, COL)].reshape(count * pcol, COL)

    def partial_sum(m, j, p):
        out = None
        for i in (2 * p, 2 * p + 1):
            first, count = seg[i]
            term = dot(hg[:, first * pcol:(first + count) * pcol], weights(m, j, i))
            out = term if out is None else out + term
        return out

    def gate_up(p, group):
        for j in group:
            gate, up = partial_sum(0, j, p), partial_sum(1, j, p)
            if p == 0:
                yb[j] = gate
                ub[j] = up
            else:
                gate = yb[j] + gate
                gate = 0.5 * gate * (1.0 + jnp.tanh(0.5 * gate))
                u[:, cols(core * half + j * COL, COL)] = (gate * (ub[j] + up)).astype(BF16)
        if p == 1:
            for j in group:
                here = u.at[:, cols(core * half + j * COL, COL)]
                send(here, here, u_send.at[j], u_recv.at[j], mate)

    def gate_up_part(p):
        for i in (2 * p, 2 * p + 1):
            first, count = seg[i]
            for m, (w_buf, tail) in enumerate(((wg, kbuf), (wu, vbuf))):
                landed(w_buf.at[pl.ds(first, count)], gu_sem.at[m, i])
                for t in range(n_tail):
                    landed(tail.at[pl.ds(t * prow + first, count)], tail_sem.at[m, t, i])
        phase('gateup%d' % p)

        if p == 0:
            gate_up(p, range(n_col - 2))
            phase('gather2')
            for i in (2, 3, 4, 5):
                take(1, i)
            phase('gateup0b')
            gate_up(p, range(n_col - 2, n_col))
        else:
            gate_up(p, range(3))
            gate_up(p, range(3, 5))
            gate_up(p, range(5, n_col))

    take(0, 0)
    take(0, 1)
    hop_own(1, True)
    phase('gather_b')
    for p, i in ((0, 2), (0, 3), (1, 0), (1, 1)):
        take(p, i)
    phase('gather_c')
    for p, i in ((0, 4), (0, 5)):
        take(p, i)
    from_mate(0)
    phase('wait_gu0')
    gate_up_part(0)
    phase('gather3')
    from_mate(1)
    phase('wait_gu1')
    gate_up_part(1)
    phase('down0')
    ahead = 1
    fold_half = half // pcol

    def down_half(whose, group):
        at = pl.ds(whose * fold_half, fold_half)
        part = slice(group[0] * COL, (group[-1] + 1) * COL)
        return dot(u[:, cols(whose * half, half)], wa[at, :, part].reshape(half, len(group) * COL))

    def keep(group, value, add):
        for n, j in enumerate(group):
            piece_of = value[:, n * COL:(n + 1) * COL]
            yb[j] = yb[j] + piece_of if add else piece_of

    pairs = [range(j, min(j + 2, n_col)) for j in range(0, n_col, 2)]
    for group in pairs[:ahead]:
        for j in group:
            landed(wa.at[:, :, 0:COL], wd_sem.at[j])
        keep(group, down_half(core, group), False)

    phase('wait_u')
    for j in range(n_col):
        arrived(u.at[:, cols((1 - core) * half + j * COL, COL)], u_recv.at[j])

    phase('down')
    def way(j):
        sign = (1 - 2 * core) * (1 - 2 * (j % 2))
        return sign

    def rows_of(owner):
        return pl.ds(pl.multiple_of(lax.rem(owner + 2 * n_dev, n_dev) * rows, rows), rows)

    def pass_far(j):
        send(yb.at[j, rows_of(dev + 2)], r1.at[j], rs_send.at[0, j], rs_recv.at[0, j], on_y(way(j)))

    def pass_near(j):
        sign = way(j)
        send(yb.at[j, rows_of(dev - sign)], r3.at[j], rs_send.at[2, j], rs_recv.at[2, j], on_y(-sign))

    def pass_sum(j):
        sign = way(j)
        arrived(r1.at[j], rs_recv.at[0, j])
        yb[j, rows_of(dev + sign), :] += r1[j]
        send(yb.at[j, rows_of(dev + sign)], r2.at[j], rs_send.at[1, j], rs_recv.at[1, j], on_y(sign))

    for i, group in enumerate(pairs):
        if i < ahead:
            keep(group, down_half(1 - core, group), True)
        else:
            for j in group:
                landed(wa.at[:, :, 0:COL], wd_sem.at[j])
            part = slice(group[0] * COL, (group[-1] + 1) * COL)
            keep(group, dot(u[...], wa[:, :, part].reshape(prow * pcol, len(group) * COL)), False)
        for j in group:
            pass_far(j)

    phase('stage2')
    for j in range(n_col):
        pass_near(j)
    for j in range(n_col):
        pass_sum(j)

    phase('final')
    blk = rows // CORES
    my_blk = pl.ds(pl.multiple_of(core * blk, blk), blk)
    mate_blk = pl.ds(pl.multiple_of((1 - core) * blk, blk), blk)
    for j in range(n_col):
        arrived(r2.at[j], rs_recv.at[1, j])
        arrived(r3.at[j], rs_recv.at[2, j])
        y = (yb[j, rows_of(dev), :] + r2[j] + r3[j]).astype(BF16)
        here = cols(core * half + j * COL, COL)
        fin[j] = (x1b[:, here].astype(F32) + y.astype(F32)).astype(BF16)
        send(fin.at[j, mate_blk], out_hbm.at[:, here], fin_send.at[j], fin_recv.at[j], mate)
        load(fin.at[j, my_blk], out_hbm.at[:, here], out_sem.at[j], 0)
    phase('fin')
    for j in range(n_col):
        arrived(out_hbm.at[:, cols((1 - core) * half + j * COL, COL)], fin_recv.at[j])
    phase('drain')
    for r in range(1, n_x):
        arrived(og.at[r], a2a_send.at[r])
    for i in range(2):
        part = slice(i * half, (i + 1) * half)
        arrived(precv.at[:, part], pp_send.at[i])
    for p in range(2):
        for i in range(12):
            strip = strips[p][(0, 1, 1, 0, 0, 1, 0, 1, 1, 0, 0, 1)[i]]
            arrived(piece(dev, strip, core), ag_send.at[p, i])
    for j in range(n_col):
        arrived(u.at[:, 0:COL], u_send.at[j])
        for i in range(3):
            arrived(r1.at[0], rs_send.at[i, j])
    for j in range(n_col):
        arrived(fin.at[j, mate_blk], fin_send.at[j])
        arrived(fin.at[j, my_blk], out_sem.at[j])
    phase(None)


def solution(mesh):
    n_side = mesh.shape['side']
    n_dev = mesh.shape['dev']
    batch_axes = ('inst', 'dev')
    in_specs = (
        P(batch_axes, None),
        P(batch_axes),
        P(None, batch_axes, None, None, None),
        P(None, batch_axes, None, None, None),
        P(), P(), P(), P(), P(),
        P(None, None, 'dev'),
        P(None, None, 'dev'),
        P(None, 'dev', None),
    )
    out_specs = P(('inst', 'dev', 'side'), None)

    def device_fn(hidden, cache_len, k_cache, v_cache, w_q, w_kv, w_o, attn_gain, ffn_gain, w_gate, w_up, w_down):
        seqs, width = hidden.shape
        span, head = k_cache.shape[3:]
        ff = w_gate.shape[2]
        half = width // 2
        rows = seqs * CORES // n_side
        n_x = n_side // CORES
        n_col = half // COL
        q_cols = w_q.shape[2] // n_side
        tall = width // span
        freqs = jnp.asarray(ROPE_BASE ** (-np.arange(head // 2, dtype=np.float64) / (head // 2)), F32)[None]

        def fold(w):
            return w.reshape(w.shape[1] // span, span, w.shape[2])

        args = (hidden, cache_len.reshape(1, seqs), freqs, k_cache[0], v_cache[0], fold(w_q), fold(w_kv),
                w_o.reshape(n_side, w_o.shape[1] // n_side, width), attn_gain, ffn_gain,
                fold(w_gate), fold(w_up), fold(w_down))
        vmem = pltpu.VMEM
        dma = pltpu.SemaphoreType.DMA
        main = ff // CORES - 2 * COL
        scratch = [
            vmem((seqs, width), BF16), vmem((1, seqs), jnp.int32), vmem((1, head // 2), F32),
            vmem((1, width), F32), vmem((1, width), F32), vmem((rows, width), BF16),
            vmem((tall, span, half), BF16),
            vmem((seqs, span, head), BF16), vmem((seqs, span, head), BF16),
            vmem((n_x, q_cols, width), BF16),
            vmem((tall, span, main), BF16), vmem((tall, span, main), BF16),
            vmem((n_col, seqs, COL), F32), vmem((n_col, seqs, COL), F32), vmem((seqs, 1), F32),
            vmem((seqs, q_cols), BF16), vmem((n_x, rows, q_cols), BF16),
            vmem((rows, width), F32), vmem((rows, width), F32), vmem((rows, width), BF16),
            vmem((n_dev * rows, width), BF16), vmem((seqs, ff), BF16),
            vmem((n_col, rows, COL), F32), vmem((n_col, rows, COL), F32), vmem((n_col, rows, COL), F32),
            vmem((n_col, rows, COL), BF16),
            dma((6,)), dma((4,)), dma((2, n_x)), dma((n_x,)), dma((2, 4)), dma((2, 2, 4)), dma((n_col,)), dma((n_col,)),
            dma((n_x,)), dma((n_x,)), dma((2,)), dma((2,)), dma((2, 12)), dma((2, 12)), dma((n_col,)), dma((n_col,)),
            dma((3, n_col)), dma((3, n_col)), dma((n_col,)), dma((n_col,)),
        ]
        anywhere = pl.BlockSpec(memory_space=pl.ANY)
        return pl.pallas_call(
            functools.partial(layer_kernel, n_dev, n_side),
            out_shape=jax.ShapeDtypeStruct((rows // CORES, width), BF16),
            in_specs=[anywhere] * len(args),
            out_specs=anywhere,
            scratch_shapes=scratch,
            compiler_params=pltpu.CompilerParams(
                collective_id=0, has_side_effects=True, vmem_limit_bytes=67_043_328),
        )(*args)

    return jax.shard_map(device_fn, mesh=mesh, in_specs=in_specs, out_specs=out_specs, check_vma=False)
```

```python
import functools

import jax
import jax.numpy as jnp
import numpy as np
from jax import lax
from jax.experimental import pallas as pl
from jax.experimental.pallas import tpu as pltpu
from jax.sharding import PartitionSpec as P

EPS = 1e-5
ROPE_BASE = 10000.0
MESH = pl.DeviceIdType.MESH
F32 = jnp.float32
BF16 = jnp.bfloat16
COL = 256
CORES = 2
NEG = -1e30


def dot(lhs, rhs):
    return jnp.dot(lhs, rhs, preferred_element_type=F32)


def rms_scale(square_sum, width):
    return lax.rsqrt(square_sum / width + EPS)


def square_sums(parts):
    acc = None
    for part in parts:
        for g in range(part.shape[1] // 128):
            x = part[:, g * 128:(g + 1) * 128]
            acc = x * x if acc is None else acc + x * x
    return jnp.sum(acc, axis=1, keepdims=True)


def pair_blocks(first, second):
    rows, n = first.shape
    both = jnp.concatenate([first.reshape(rows // 8, 8, n), second.reshape(rows // 8, 8, n)], axis=1)
    return both.reshape(2 * rows, n)


class Phases:
    def __init__(self):
        self.scope = None

    def __call__(self, name):
        if self.scope is not None:
            self.scope.__exit__(None, None, None)
        self.scope = None if name is None else jax.named_scope(name)
        if self.scope is not None:
            self.scope.__enter__()


def layer_kernel(n_dev, n_side,
                 x_hbm, len_hbm, freq_hbm, k_hbm, v_hbm, wq_hbm, wkv_hbm, wo_hbm, again_hbm, fgain_hbm,
                 wg_hbm, wu_hbm, wd_hbm, out,
                 act, lens, freqs, again, fgain, xres, wa, kbuf, vbuf, wo, wg, wu,
                 yb, ub, lenc, osend, og, pp, precv, x1b, hg, u, r1, r2, r3, r4,
                 in_sem, w_sem, kv_sem, wo_sem, gu_sem, tail_sem, wd_sem,
                 a2a_send, a2a_recv, pp_send, pp_recv, ag_send, ag_recv, u_send, u_recv,
                 rs_send, rs_recv, fin_send, fin_recv):
    dev = lax.axis_index('dev')
    side = lax.axis_index('side')
    n_x = n_side // CORES
    chip = lax.div(side, CORES)
    core = lax.rem(side, CORES)
    mate = {'side': CORES * chip + 1 - core}
    seqs, width = act.shape
    head = COL
    q_cols = osend.shape[1]
    half = width // 2
    rows = xres.shape[0]
    n_col = half // COL
    kq = n_col // 2 * COL // wa.shape[1]
    n_main = wg.shape[2] // COL
    n_tail = n_col - n_main
    kv_half = wkv_hbm.shape[2] // 2
    prow, pcol = wa.shape[0], wa.shape[1]

    def on_x(r):
        return {'side': CORES * lax.rem(chip + r, n_x) + 1 - core}

    def on_y(r):
        return {'dev': lax.rem(dev + r + n_dev, n_dev)}

    phase = Phases()
    phase('start')
    barrier = pltpu.get_barrier_semaphore()
    peers = [mate] + [on_x(r) for r in range(1, n_x)] + [on_y(1), on_y(-1)]
    peers += [{**on_y(1), **mate}, {**on_y(-1), **mate}]
    for peer in peers:
        pl.semaphore_signal(barrier, inc=1, device_id=peer, device_id_type=MESH)

    def cols(start, size):
        return pl.ds(pl.multiple_of(start, 128), size)

    def load(src, dst, sem, priority=1):
        pltpu.make_async_copy(src, dst, sem).start(priority=priority)

    def landed(dst, sem):
        pltpu.make_async_copy(dst, dst, sem).wait()

    cut = (n_col + 1) // 2 * 2 * COL
    spans = (slice(0, cut), slice(cut, width))
    my_rows = pl.ds(pl.multiple_of(chip * rows, rows), rows)

    load(x_hbm, act, in_sem.at[0], 0)
    load(len_hbm, lens, in_sem.at[1], 0)
    load(freq_hbm, freqs, in_sem.at[2], 0)
    load(again_hbm, again, in_sem.at[3], 0)
    load(fgain_hbm, fgain, in_sem.at[4], 0)
    load(x_hbm.at[my_rows], xres, in_sem.at[5], 0)

    def w_slot(j):
        return wa.at[:, :, j * COL:(j + 1) * COL]

    load(wq_hbm.at[:, :, cols(side * q_cols, COL)], w_slot(0), w_sem.at[0])
    load(wq_hbm.at[:, :, cols(side * q_cols + COL, COL)], w_slot(1), w_sem.at[1])
    load(wkv_hbm.at[:, :, cols(side * head, COL)], w_slot(2), w_sem.at[2])
    load(wkv_hbm.at[:, :, cols(kv_half + side * head, COL)], w_slot(3), w_sem.at[3])
    phase('wait_x')
    for i, ref in enumerate((act, lens, freqs, again, fgain, xres)):
        landed(ref, in_sem.at[i])
    by_distance = sorted(range(1, n_x), key=lambda r: (-min(r, n_x - r), -r)) + [0]

    def cache_rows(r):
        return pl.ds(lax.rem(chip + r, n_x) * rows, rows)

    def load_cache(r):
        at = cache_rows(r)
        load(k_hbm.at[at, side], kbuf.at[at], kv_sem.at[0, r])
        load(v_hbm.at[at, side], vbuf.at[at], kv_sem.at[1, r])

    order = [0] + by_distance[1:-1] + by_distance[:1]

    def slot(r):
        start = order.index(r) * q_cols
        return slice(start, start + q_cols)

    def wo_slot(r):
        return wo.at[slot(r)]

    def load_wo(r):
        src_core = core if r == 0 else 1 - core
        load(wo_hbm.at[CORES * lax.rem(chip + n_x - r, n_x) + src_core], wo_slot(r), wo_sem.at[r])

    load_cache(by_distance[0])
    phase('tables')
    row_id = lax.broadcasted_iota(jnp.int32, (seqs, seqs), 0)
    col_id = lax.broadcasted_iota(jnp.int32, (seqs, seqs), 1)
    wide = jnp.broadcast_to(lens[...].astype(F32), (seqs, seqs))
    len_col = jnp.sum(jnp.where(row_id == col_id, wide, 0.0), axis=1, keepdims=True)
    angle = len_col * freqs[...]
    cos_part = jnp.cos(angle)
    sin_part = jnp.sin(angle)

    def rotate(vecs):
        first, second = vecs[:, :head // 2], vecs[:, head // 2:]
        return jnp.concatenate([first * cos_part - second * sin_part, second * cos_part + first * sin_part], axis=1)

    phase('norm1')
    inv = rms_scale(square_sums([act[:, i * COL:(i + 1) * COL].astype(F32) for i in range(2 * n_col)]), width)
    for i in range(2 * n_col):
        part = slice(i * COL, (i + 1) * COL)
        act[:, part] = (act[:, part].astype(F32) * inv * again[:, part]).astype(BF16)

    phase('qkv')
    lenc[...] = len_col

    for j in range(4):
        landed(w_slot(0), w_sem.at[j])
        if j + 1 < n_x:
            load_cache(by_distance[j + 1])
        yb[j] = dot(act[...], wa[:, :, cols(j * COL, COL)].reshape(prow * pcol, COL))

    load_wo(0)
    load_wo(by_distance[1])
    phase('rope')
    for j in range(4):
        vecs = yb[j] if j == 3 else rotate(yb[j])
        yb[j] = vecs.astype(BF16).astype(F32)

    span = kbuf.shape[1]
    keys = 8 * span
    scale = head ** -0.5
    groups = rows // 8
    row = lax.broadcasted_iota(jnp.int32, (2 * rows, keys), 0)
    key = lax.broadcasted_iota(jnp.int32, (2 * rows, keys), 1)
    offset = key - lax.rem(row, 8) * span

    def cat(parts):
        return parts[0] if len(parts) == 1 else jnp.concatenate(parts, axis=0)

    def attend(theres):
        ats = [pl.ds(pl.multiple_of(there * rows, rows), rows) for there in theres]
        q0, q1, k_new, v_new = (cat([yb[j, at, :] for at in ats]) for j in range(4))
        q_pair = pair_blocks(q0, q1).astype(BF16)
        self_score = pair_blocks(jnp.sum(q0 * k_new, axis=1, keepdims=True),
                                 jnp.sum(q1 * k_new, axis=1, keepdims=True)) * scale
        lengths = cat([lenc[at, :] for at in ats])
        len_rows = pair_blocks(lengths, lengths).astype(jnp.int32)
        blocks = [there * rows + 8 * b for there in theres for b in range(groups)]
        scores = cat([
            lax.dot_general(q_pair[16 * n:16 * n + 16], kbuf[pl.ds(b, 8)].reshape(keys, head),
                            (((1,), (1,)), ((), ())), preferred_element_type=F32)
            for n, b in enumerate(blocks)])
        offsets = cat([offset] * len(theres))
        scores = jnp.where((offsets >= 0) & (offsets < len_rows), scores * scale, NEG)
        row_max = jnp.maximum(jnp.max(scores, axis=1, keepdims=True), self_score)
        exp_scores = jnp.exp(scores - row_max)
        self_exp = jnp.exp(self_score - row_max)
        total = jnp.sum(exp_scores, axis=1, keepdims=True) + self_exp
        probs = exp_scores.astype(BF16)
        mixed = cat([dot(probs[16 * n:16 * n + 16], vbuf[pl.ds(b, 8)].reshape(keys, head))
                     for n, b in enumerate(blocks)])
        mixed = mixed + self_exp.astype(BF16).astype(F32) * pair_blocks(v_new, v_new)
        mixed = (mixed / total).reshape(len(blocks), 16, head)
        first = mixed[:, :8].reshape(len(theres) * rows, head).astype(BF16)
        second = mixed[:, 8:].reshape(len(theres) * rows, head).astype(BF16)
        for n, at in enumerate(ats):
            osend[at, :head] = first[n * rows:(n + 1) * rows]
            osend[at, head:] = second[n * rows:(n + 1) * rows]
        return ats

    def send(src, dst, send_sem, recv_sem, where):
        pltpu.make_async_remote_copy(src, dst, send_sem, recv_sem, device_id=where, device_id_type=MESH).start()

    def arrived(dst, sem):
        pltpu.make_async_copy(dst, dst, sem).wait()

    def og_slot(r):
        return og.at[:, slot(r)]

    pl.semaphore_wait(barrier, len(peers))
    for pair in (by_distance[:2], by_distance[2:3], by_distance[3:]):
        phase('wait_kv%d' % pair[0])
        for r in pair:
            landed(kbuf.at[cache_rows(r)], kv_sem.at[0, r])
            landed(vbuf.at[cache_rows(r)], kv_sem.at[1, r])
        phase('attend%d' % pair[0])
        ats = attend([lax.rem(chip + r, n_x) for r in pair])
        for r, at in zip(pair, ats):
            if r:
                send(osend.at[at], og_slot(r), a2a_send.at[r], a2a_recv.at[r], on_x(r))
        if pair[0] == by_distance[0]:
            load_wo(by_distance[0])
            load_wo(by_distance[2])

    phase('loads2')
    seg = ((0, kq), (half // pcol, kq), (kq, half // pcol - kq), (half // pcol + kq, half // pcol - kq))

    def load_gate_up(part):
        for i in (2 * part, 2 * part + 1):
            first, count = seg[i]
            at = pl.ds(first, count)
            for m, (w_hbm, w_buf, tail) in enumerate(((wg_hbm, wg, kbuf), (wu_hbm, wu, vbuf))):
                load(w_hbm.at[at, :, cols(core * half, n_main * COL)], w_buf.at[at], gu_sem.at[m, i])
                for t in range(n_tail):
                    load(w_hbm.at[at, :, cols(core * half + (n_main + t) * COL, COL)],
                         tail.at[pl.ds(t * prow + first, count)], tail_sem.at[m, t, i])

    load_gate_up(0)
    load_gate_up(1)
    phase('proj')
    phase('proj0')
    landed(wo_slot(0), wo_sem.at[0])
    pp[...] = dot(osend[my_rows, :], wo[0:q_cols, :])
    def wait_heads(r):
        landed(wo_slot(r), wo_sem.at[r])
        arrived(og_slot(r), a2a_recv.at[r])

    phase('proj1')
    wait_heads(order[1])
    pp[...] += dot(og[:, slot(order[1])], wo[slot(order[1]), :])
    phase('wait_proj')
    for r in order[2:]:
        wait_heads(r)
    phase('proj_rest')
    for i, part in enumerate(spans):
        pp[:, part] += dot(og[:, 2 * q_cols:], wo[2 * q_cols:, part])
        send(pp.at[:, part], precv.at[:, part], pp_send.at[i], pp_recv.at[i], mate)
    for j in range(n_col):
        load(wd_hbm.at[:, :, cols(core * half + j * COL, COL)], wa.at[:, :, j * COL:(j + 1) * COL], wd_sem.at[j])

    phase('wait_mate')
    dev_rows = pl.ds(pl.multiple_of(dev * rows, rows), rows)
    for i, part in enumerate(spans):
        arrived(precv.at[:, part], pp_recv.at[i])
        x1b[:, part] = (xres[:, part].astype(F32) + (pp[:, part] + precv[:, part])).astype(BF16)
    phase('norm2')
    inv2 = rms_scale(square_sums([x1b[:, i * COL:(i + 1) * COL].astype(F32) for i in range(2 * n_col)]), width)
    for i in range(2 * n_col):
        part = slice(i * COL, (i + 1) * COL)
        hg[dev_rows, part] = (x1b[:, part].astype(F32) * inv2 * fgain[:, part]).astype(BF16)

    phase('gather')
    ka = kq * pcol // 2
    kb = (half - kq * pcol) // 2
    strips = (((0, ka), (ka, ka)), ((2 * ka, kb), (2 * ka + kb, kb)))

    def piece(owner, strip, whose):
        owner_rows = pl.ds(pl.multiple_of(lax.rem(owner + 2 * n_dev, n_dev) * rows, rows), rows)
        return hg.at[owner_rows, cols(whose * half + strip[0], strip[1])]

    def across(step):
        return {**on_y(step), **mate}

    def hop(owner, strip, p, i, where, whose):
        ref = piece(owner, strip, whose)
        send(ref, ref, ag_send.at[p, i], ag_recv.at[p, i], where)

    source = ((-1, 0), (1, 1), (-1, 1), (1, 0), (2, 0), (2, 1))
    def hop_own(p, late):
        if late:
            hop(dev, strips[p][1], p, 2, across(1), core)
            hop(dev, strips[p][0], p, 3, across(-1), core)
        else:
            hop(dev, strips[p][0], p, 0, across(1), core)
            hop(dev, strips[p][1], p, 1, across(-1), core)

    hop_own(0, False)
    hop_own(0, True)
    hop_own(1, False)

    def take_near(p, i):
        owner = dev + 2 * i - 1
        start = strips[p][0][0] + i * strips[p][0][1]
        ref = piece(owner, (start, strips[p][0][1]), 1 - core)
        arrived(ref, ag_recv.at[p, i])
        send(ref, ref, ag_send.at[p, 4 + i], ag_recv.at[p, 4 + i], across(1 - 2 * i))
        send(ref, ref, ag_send.at[p, 6 + i], ag_recv.at[p, 6 + i], mate)

    def take(p, i):
        owner, strip = dev + source[i][0], strips[p][source[i][1]]
        whose = 1 - core if i < 4 else core
        arrived(piece(owner, strip, whose), ag_recv.at[p, i])
        hop(owner, strip, p, 6 + i, mate, whose)

    def from_mate(p):
        for i in range(6):
            owner, strip = dev + source[i][0], strips[p][source[i][1]]
            arrived(piece(owner, strip, core if i < 4 else 1 - core), ag_recv.at[p, 6 + i])

    def weights(m, j, i):
        first, count = seg[i]
        main, tail = (wg, kbuf) if m == 0 else (wu, vbuf)
        if isinstance(j, int) and j >= n_main:
            start = (j - n_main) * prow + first
            return tail[start:start + count].reshape(count * pcol, COL)
        return main[first:first + count, :, cols(j * COL, COL)].reshape(count * pcol, COL)

    def partial_sum(m, j, p):
        out = None
        for i in (2 * p, 2 * p + 1):
            first, count = seg[i]
            term = dot(hg[:, first * pcol:(first + count) * pcol], weights(m, j, i))
            out = term if out is None else out + term
        return out

    def gate_up(p, group):
        for j in group:
            gate, up = partial_sum(0, j, p), partial_sum(1, j, p)
            if p == 0:
                yb[j] = gate
                ub[j] = up
            else:
                gate = yb[j] + gate
                gate = 0.5 * gate * (1.0 + jnp.tanh(0.5 * gate))
                u[:, cols(core * half + j * COL, COL)] = (gate * (ub[j] + up)).astype(BF16)
        if p == 1:
            for j in group:
                here = u.at[:, cols(core * half + j * COL, COL)]
                send(here, here, u_send.at[j], u_recv.at[j], mate)

    def gate_up_part(p):
        for i in (2 * p, 2 * p + 1):
            first, count = seg[i]
            for m, (w_buf, tail) in enumerate(((wg, kbuf), (wu, vbuf))):
                landed(w_buf.at[pl.ds(first, count)], gu_sem.at[m, i])
                for t in range(n_tail):
                    landed(tail.at[pl.ds(t * prow + first, count)], tail_sem.at[m, t, i])
        phase('gateup%d' % p)

        if p == 0:
            gate_up(p, range(n_col - 4))
            phase('gather2')
            for i in (2, 3, 4, 5):
                take(1, i)
            phase('gateup0b')
            gate_up(p, range(n_col - 4, n_col))
        else:
            gate_up(p, range(n_col - 3))
            gate_up(p, range(n_col - 3, n_col - 1))
            gate_up(p, range(n_col - 1, n_col))

    near = 1 - jnp.minimum(dev, 1)
    take_near(0, near)
    take_near(0, 1 - near)
    hop_own(1, True)
    phase('gather_b')
    take(0, 2)
    take(0, 3)
    take_near(1, near)
    take_near(1, 1 - near)
    phase('gather_c')
    for p, i in ((0, 4), (0, 5)):
        take(p, i)
    from_mate(0)
    phase('wait_gu0')
    gate_up_part(0)
    phase('gather3')
    from_mate(1)
    phase('wait_gu1')
    gate_up_part(1)
    phase('down0')
    fold_half = half // pcol

    def down_half(whose, group):
        at = pl.ds(whose * fold_half, fold_half)
        part = slice(group[0] * COL, (group[-1] + 1) * COL)
        return dot(u[:, cols(whose * half, half)], wa[at, :, part].reshape(half, len(group) * COL))

    def keep(group, value, add):
        for n, j in enumerate(group):
            piece_of = value[:, n * COL:(n + 1) * COL]
            yb[j] = yb[j] + piece_of if add else piece_of

    pairs = [range(j, min(j + 2, n_col)) for j in range(0, n_col, 2)]
    for j in range(n_col):
        landed(wa.at[:, :, 0:COL], wd_sem.at[j])
    for group in pairs[:2]:
        keep(group, down_half(core, group), False)

    phase('wait_u')
    for j in range(n_col):
        arrived(u.at[:, cols((1 - core) * half + j * COL, COL)], u_recv.at[j])

    phase('down')
    def way(j):
        sign = (1 - 2 * core) * (1 - 2 * (j % 2))
        return sign

    def rows_of(owner):
        return pl.ds(pl.multiple_of(lax.rem(owner + 2 * n_dev, n_dev) * rows, rows), rows)

    blk = rows // CORES
    sides = [{'side': CORES * chip + b} for b in range(CORES)]

    def block_of(owner, b):
        start = lax.rem(owner + 2 * n_dev, n_dev) * rows + b * blk
        return pl.ds(pl.multiple_of(start, blk), blk)

    def pass_far(j):
        send(yb.at[j, rows_of(dev + 2)], r1.at[j], rs_send.at[0, 0, j], rs_recv.at[0, 0, j], on_y(way(j)))

    def pass_near(j):
        sign = way(j)
        for b in range(CORES):
            send(yb.at[j, block_of(dev - sign, b)], r3.at[core, j], rs_send.at[2, b, j], rs_recv.at[2, core, j],
                 {**on_y(-sign), **sides[b]})

    def pass_sum(j):
        sign = way(j)
        arrived(r1.at[j], rs_recv.at[0, 0, j])
        yb[j, rows_of(dev + sign), :] += r1[j]
        for b in range(CORES):
            send(yb.at[j, block_of(dev + sign, b)], r2.at[core, j], rs_send.at[1, b, j], rs_recv.at[1, core, j],
                 {**on_y(sign), **sides[b]})

    for group in pairs:
        if group in pairs[:2]:
            keep(group, down_half(1 - core, group), True)
        else:
            part = slice(group[0] * COL, (group[-1] + 1) * COL)
            keep(group, dot(u[...], wa[:, :, part].reshape(prow * pcol, len(group) * COL)), False)
        for j in group:
            pass_far(j)

    phase('stage2')
    for j in range(n_col):
        pass_near(j)
    for j in range(n_col):
        send(yb.at[j, block_of(dev, 1 - core)], r4.at[j], fin_send.at[j], fin_recv.at[j], mate)
    for j in range(n_col):
        pass_sum(j)

    phase('final')
    my_blk = pl.ds(pl.multiple_of(core * blk, blk), blk)

    def finish(whose, j, own_sum):
        arrived(r3.at[whose, j], rs_recv.at[2, whose, j])
        arrived(r2.at[whose, j], rs_recv.at[1, whose, j])
        y = (own_sum + r2[whose, j] + r3[whose, j]).astype(BF16)
        here = cols(whose * half + j * COL, COL)
        out[:, here] = (x1b[my_blk, here].astype(F32) + y.astype(F32)).astype(BF16)

    for j in range(n_col):
        arrived(r4.at[j], fin_recv.at[j])
        finish(core, j, yb[j, block_of(dev, core), :])
        finish(1 - core, j, r4[j])
    phase('drain')
    for r in range(1, n_x):
        arrived(og_slot(r), a2a_send.at[r])
    for i, part in enumerate(spans):
        arrived(precv.at[:, part], pp_send.at[i])
    for p in range(2):
        for i in range(12):
            strip = strips[p][(0, 1, 1, 0, 0, 1, 0, 1, 1, 0, 0, 1)[i]]
            arrived(piece(dev, strip, core), ag_send.at[p, i])
    for j in range(n_col):
        arrived(u.at[:, 0:COL], u_send.at[j])
        arrived(r1.at[0], rs_send.at[0, 0, j])
        for b in range(CORES):
            arrived(r2.at[0, 0], rs_send.at[1, b, j])
            arrived(r3.at[0, 0], rs_send.at[2, b, j])
    for j in range(n_col):
        arrived(r4.at[j], fin_send.at[j])
    phase(None)


def solution(mesh):
    n_side = mesh.shape['side']
    n_dev = mesh.shape['dev']
    batch_axes = ('inst', 'dev')
    in_specs = (
        P(batch_axes, None),
        P(batch_axes),
        P(None, batch_axes, None, None, None),
        P(None, batch_axes, None, None, None),
        P(), P(), P(), P(), P(),
        P(None, None, 'dev'),
        P(None, None, 'dev'),
        P(None, 'dev', None),
    )
    out_specs = P(('inst', 'dev', 'side'), None)

    def device_fn(hidden, cache_len, k_cache, v_cache, w_q, w_kv, w_o, attn_gain, ffn_gain, w_gate, w_up, w_down):
        seqs, width = hidden.shape
        span, head = k_cache.shape[3:]
        ff = w_gate.shape[2]
        half = width // 2
        rows = seqs * CORES // n_side
        n_x = n_side // CORES
        n_col = half // COL
        q_cols = w_q.shape[2] // n_side
        tall = width // span
        freqs = jnp.asarray(ROPE_BASE ** (-np.arange(head // 2, dtype=np.float64) / (head // 2)), F32)[None]

        def fold(w):
            return w.reshape(w.shape[1] // span, span, w.shape[2])

        args = (hidden, cache_len.reshape(1, seqs), freqs, k_cache[0], v_cache[0], fold(w_q), fold(w_kv),
                w_o.reshape(n_side, w_o.shape[1] // n_side, width), attn_gain, ffn_gain,
                fold(w_gate), fold(w_up), fold(w_down))
        vmem = pltpu.VMEM
        dma = pltpu.SemaphoreType.DMA
        main = ff // CORES - 2 * COL
        scratch = [
            vmem((seqs, width), BF16), vmem((1, seqs), jnp.int32), vmem((1, head // 2), F32),
            vmem((1, width), F32), vmem((1, width), F32), vmem((rows, width), BF16),
            vmem((tall, span, half), BF16),
            vmem((seqs, span, head), BF16), vmem((seqs, span, head), BF16),
            vmem((n_x * q_cols, width), BF16),
            vmem((tall, span, main), BF16), vmem((tall, span, main), BF16),
            vmem((n_col, seqs, COL), F32), vmem((n_col, seqs, COL), F32), vmem((seqs, 1), F32),
            vmem((seqs, q_cols), BF16), vmem((rows, n_x * q_cols), BF16),
            vmem((rows, width), F32), vmem((rows, width), F32), vmem((rows, width), BF16),
            vmem((n_dev * rows, width), BF16), vmem((seqs, ff), BF16),
            vmem((n_col, rows, COL), F32), vmem((CORES, n_col, rows // CORES, COL), F32),
            vmem((CORES, n_col, rows // CORES, COL), F32), vmem((n_col, rows // CORES, COL), F32),
            dma((6,)), dma((4,)), dma((2, n_x)), dma((n_x,)), dma((2, 4)), dma((2, 2, 4)), dma((n_col,)),
            dma((n_x,)), dma((n_x,)), dma((2,)), dma((2,)), dma((2, 12)), dma((2, 12)), dma((n_col,)), dma((n_col,)),
            dma((3, CORES, n_col)), dma((3, CORES, n_col)), dma((n_col,)), dma((n_col,)),
        ]
        anywhere = pl.BlockSpec(memory_space=pl.ANY)
        return pl.pallas_call(
            functools.partial(layer_kernel, n_dev, n_side),
            out_shape=jax.ShapeDtypeStruct((rows // CORES, width), BF16),
            in_specs=[anywhere] * len(args),
            out_specs=pl.BlockSpec(memory_space=pltpu.VMEM),
            scratch_shapes=scratch,
            compiler_params=pltpu.CompilerParams(
                collective_id=0, has_side_effects=True, vmem_limit_bytes=67_043_328),
        )(*args)

    return jax.shard_map(device_fn, mesh=mesh, in_specs=in_specs, out_specs=out_specs, check_vma=False)
```

```python
import functools

import jax
import jax.numpy as jnp
import numpy as np
from jax import lax
from jax.experimental import pallas as pl
from jax.experimental.pallas import tpu as pltpu
from jax.sharding import PartitionSpec as P

EPS = 1e-5
ROPE_BASE = 10000.0
MESH = pl.DeviceIdType.MESH
F32 = jnp.float32
BF16 = jnp.bfloat16
COL = 256
CORES = 2
NEG = -1e30


def dot(lhs, rhs):
    return jnp.dot(lhs, rhs, preferred_element_type=F32)


def rms_scale(square_sum, width):
    return lax.rsqrt(square_sum / width + EPS)


def square_sums(parts):
    acc = None
    for part in parts:
        for g in range(part.shape[1] // 128):
            x = part[:, g * 128:(g + 1) * 128]
            acc = x * x if acc is None else acc + x * x
    return jnp.sum(acc, axis=1, keepdims=True)


def pair_blocks(first, second):
    rows, n = first.shape
    both = jnp.concatenate([first.reshape(rows // 8, 8, n), second.reshape(rows // 8, 8, n)], axis=1)
    return both.reshape(2 * rows, n)


class Phases:
    def __init__(self):
        self.scope = None

    def __call__(self, name):
        if self.scope is not None:
            self.scope.__exit__(None, None, None)
        self.scope = None if name is None else jax.named_scope(name)
        if self.scope is not None:
            self.scope.__enter__()


def layer_kernel(n_dev, n_side,
                 x_hbm, len_hbm, freq_hbm, k_hbm, v_hbm, wq_hbm, wkv_hbm, wo_hbm, again_hbm, fgain_hbm,
                 wg_hbm, wu_hbm, wd_hbm, out,
                 act, lens, freqs, again, fgain, xres, wa, kbuf, vbuf, wo, wg, wu,
                 yb, ub, lenc, osend, og, pp, precv, x1b, hg, u, r1, r2, r3, r4,
                 in_sem, w_sem, kv_sem, wo_sem, gu_sem, tail_sem, wd_sem,
                 a2a_send, a2a_recv, pp_send, pp_recv, ag_send, ag_recv, u_send, u_recv,
                 rs_send, rs_recv, far_recv, fin_send, fin_recv):
    dev = lax.axis_index('dev')
    side = lax.axis_index('side')
    n_x = n_side // CORES
    chip = lax.div(side, CORES)
    core = lax.rem(side, CORES)
    mate = {'side': CORES * chip + 1 - core}
    seqs, width = act.shape
    head = COL
    q_cols = osend.shape[1]
    half = width // 2
    rows = xres.shape[0]
    n_col = half // COL
    kq = n_col // 2 * COL // wa.shape[1]
    n_main = wg.shape[2] // COL
    n_tail = n_col - n_main
    kv_half = wkv_hbm.shape[2] // 2
    prow, pcol = wa.shape[0], wa.shape[1]

    def on_x(r):
        return {'side': CORES * lax.rem(chip + r, n_x) + 1 - core}

    def on_y(r):
        return {'dev': lax.rem(dev + r + n_dev, n_dev)}

    phase = Phases()
    phase('start')
    barrier = pltpu.get_barrier_semaphore()
    peers = [mate] + [on_x(r) for r in range(1, n_x)] + [on_y(1), on_y(-1)]
    peers += [{**on_y(1), **mate}, {**on_y(-1), **mate}]
    for peer in peers:
        pl.semaphore_signal(barrier, inc=1, device_id=peer, device_id_type=MESH)

    def cols(start, size):
        return pl.ds(pl.multiple_of(start, 128), size)

    def load(src, dst, sem, priority=1):
        pltpu.make_async_copy(src, dst, sem).start(priority=priority)

    def landed(dst, sem):
        pltpu.make_async_copy(dst, dst, sem).wait()

    cut = (n_col + 1) // 2 * 2 * COL
    spans = (slice(0, cut), slice(cut, width))
    my_rows = pl.ds(pl.multiple_of(chip * rows, rows), rows)

    load(x_hbm, act, in_sem.at[0], 0)
    load(len_hbm, lens, in_sem.at[1], 0)
    load(freq_hbm, freqs, in_sem.at[2], 0)
    load(again_hbm, again, in_sem.at[3], 0)
    load(fgain_hbm, fgain, in_sem.at[4], 0)
    load(x_hbm.at[my_rows], xres, in_sem.at[5], 0)

    def w_slot(j):
        return wa.at[:, :, j * COL:(j + 1) * COL]

    load(wq_hbm.at[:, :, cols(side * q_cols, COL)], w_slot(0), w_sem.at[0])
    load(wq_hbm.at[:, :, cols(side * q_cols + COL, COL)], w_slot(1), w_sem.at[1])
    load(wkv_hbm.at[:, :, cols(side * head, COL)], w_slot(2), w_sem.at[2])
    load(wkv_hbm.at[:, :, cols(kv_half + side * head, COL)], w_slot(3), w_sem.at[3])
    phase('wait_x')
    for i, ref in enumerate((act, lens, freqs, again, fgain, xres)):
        landed(ref, in_sem.at[i])
    by_distance = sorted(range(1, n_x), key=lambda r: (-min(r, n_x - r), -r)) + [0]

    def cache_rows(r):
        return pl.ds(lax.rem(chip + r, n_x) * rows, rows)

    def load_cache(r):
        at = cache_rows(r)
        group = max(by_distance.index(r) - 1, 0)
        load(k_hbm.at[at, side], kbuf.at[at], kv_sem.at[group])
        load(v_hbm.at[at, side], vbuf.at[at], kv_sem.at[group])

    order = [0] + by_distance[1:-1] + by_distance[:1]

    def slot(r):
        start = order.index(r) * q_cols
        return slice(start, start + q_cols)

    def wo_slot(r):
        return wo.at[slot(r)]

    def load_wo(r):
        src_core = core if r == 0 else 1 - core
        load(wo_hbm.at[CORES * lax.rem(chip + n_x - r, n_x) + src_core], wo_slot(r), wo_sem.at[min(order.index(r), 2)])

    load_cache(by_distance[0])
    load_cache(by_distance[1])
    phase('tables')
    row_id = lax.broadcasted_iota(jnp.int32, (seqs, seqs), 0)
    col_id = lax.broadcasted_iota(jnp.int32, (seqs, seqs), 1)
    wide = jnp.broadcast_to(lens[...].astype(F32), (seqs, seqs))
    len_col = jnp.sum(jnp.where(row_id == col_id, wide, 0.0), axis=1, keepdims=True)
    angle = len_col * freqs[...]
    cos_part = jnp.cos(angle)
    sin_part = jnp.sin(angle)

    def rotate(vecs):
        first, second = vecs[:, :head // 2], vecs[:, head // 2:]
        return jnp.concatenate([first * cos_part - second * sin_part, second * cos_part + first * sin_part], axis=1)

    phase('norm1')
    inv = rms_scale(square_sums([act[:, i * COL:(i + 1) * COL].astype(F32) for i in range(2 * n_col)]), width)
    for i in range(2 * n_col):
        part = slice(i * COL, (i + 1) * COL)
        act[:, part] = (act[:, part].astype(F32) * inv * again[:, part]).astype(BF16)

    phase('qkv')
    lenc[...] = len_col

    for j in range(4):
        landed(w_slot(0), w_sem.at[j])
        if j == 3:
            load_cache(by_distance[2])
        yb[j] = dot(act[...], wa[:, :, cols(j * COL, COL)].reshape(prow * pcol, COL))

    load_cache(by_distance[3])
    load_wo(0)
    load_wo(by_distance[1])
    phase('rope')
    for j in range(4):
        vecs = yb[j] if j == 3 else rotate(yb[j])
        yb[j] = vecs.astype(BF16).astype(F32)

    span = kbuf.shape[1]
    keys = 8 * span
    scale = head ** -0.5
    groups = rows // 8
    row = lax.broadcasted_iota(jnp.int32, (2 * rows, keys), 0)
    key = lax.broadcasted_iota(jnp.int32, (2 * rows, keys), 1)
    offset = key - lax.rem(row, 8) * span

    def cat(parts):
        return parts[0] if len(parts) == 1 else jnp.concatenate(parts, axis=0)

    def attend(theres):
        ats = [pl.ds(pl.multiple_of(there * rows, rows), rows) for there in theres]
        q0, q1, k_new, v_new = (cat([yb[j, at, :] for at in ats]) for j in range(4))
        q_pair = pair_blocks(q0, q1).astype(BF16)
        self_score = pair_blocks(jnp.sum(q0 * k_new, axis=1, keepdims=True),
                                 jnp.sum(q1 * k_new, axis=1, keepdims=True)) * scale
        lengths = cat([lenc[at, :] for at in ats])
        len_rows = pair_blocks(lengths, lengths).astype(jnp.int32)
        blocks = [there * rows + 8 * b for there in theres for b in range(groups)]
        scores = cat([
            lax.dot_general(q_pair[16 * n:16 * n + 16], kbuf[pl.ds(b, 8)].reshape(keys, head),
                            (((1,), (1,)), ((), ())), preferred_element_type=F32)
            for n, b in enumerate(blocks)])
        offsets = cat([offset] * len(theres))
        scores = jnp.where((offsets >= 0) & (offsets < len_rows), scores * scale, NEG)
        row_max = jnp.maximum(jnp.max(scores, axis=1, keepdims=True), self_score)
        exp_scores = jnp.exp(scores - row_max)
        self_exp = jnp.exp(self_score - row_max)
        total = jnp.sum(exp_scores, axis=1, keepdims=True) + self_exp
        probs = exp_scores.astype(BF16)
        mixed = cat([dot(probs[16 * n:16 * n + 16], vbuf[pl.ds(b, 8)].reshape(keys, head))
                     for n, b in enumerate(blocks)])
        mixed = mixed + self_exp.astype(BF16).astype(F32) * pair_blocks(v_new, v_new)
        mixed = (mixed / total).reshape(len(blocks), 16, head)
        first = mixed[:, :8].reshape(len(theres) * rows, head).astype(BF16)
        second = mixed[:, 8:].reshape(len(theres) * rows, head).astype(BF16)
        for n, at in enumerate(ats):
            osend[at, :head] = first[n * rows:(n + 1) * rows]
            osend[at, head:] = second[n * rows:(n + 1) * rows]
        return ats

    def send(src, dst, send_sem, recv_sem, where):
        pltpu.make_async_remote_copy(src, dst, send_sem, recv_sem, device_id=where, device_id_type=MESH).start()

    def arrived(dst, sem):
        pltpu.make_async_copy(dst, dst, sem).wait()

    def og_slot(r):
        return og.at[:, slot(r)]

    pl.semaphore_wait(barrier, len(peers))
    for group, pair in enumerate((by_distance[:2], by_distance[2:3], by_distance[3:])):
        phase('wait_kv%d' % pair[0])
        landed(kbuf.at[pl.ds(0, 2 * len(pair) * rows)], kv_sem.at[group])
        phase('attend%d' % pair[0])
        ats = attend([lax.rem(chip + r, n_x) for r in pair])
        for r, at in zip(pair, ats):
            if r:
                send(osend.at[at], og_slot(r), a2a_send.at[0], a2a_recv.at[min(order.index(r), 2)], on_x(r))
        if pair[0] == by_distance[0]:
            load_wo(by_distance[0])
            load_wo(by_distance[2])

    phase('loads2')
    seg = ((0, kq), (half // pcol, kq), (kq, half // pcol - kq), (half // pcol + kq, half // pcol - kq))

    def load_gate_up(part):
        for i in (2 * part, 2 * part + 1):
            first, count = seg[i]
            at = pl.ds(first, count)
            for m, (w_hbm, w_buf, tail) in enumerate(((wg_hbm, wg, kbuf), (wu_hbm, wu, vbuf))):
                load(w_hbm.at[at, :, cols(core * half, n_main * COL)], w_buf.at[at], gu_sem.at[m, part])
                for t in range(n_tail):
                    load(w_hbm.at[at, :, cols(core * half + (n_main + t) * COL, COL)],
                         tail.at[pl.ds(t * prow + first, count)], tail_sem.at[m, part])

    load_gate_up(0)
    load_gate_up(1)
    phase('proj')
    def tall_dot(lhs, rhs):
        return dot(jnp.concatenate([lhs] * 4, axis=0), rhs)[:rows]

    phase('proj0')
    landed(wo_slot(0), wo_sem.at[0])
    pp[...] = dot(osend[my_rows, :], wo[0:q_cols, :])
    rest = slice(2 * q_cols, n_x * q_cols)
    phase('proj1')
    landed(wo_slot(order[1]), wo_sem.at[1])
    arrived(og_slot(order[1]), a2a_recv.at[1])
    pp[...] += tall_dot(og[:, slot(order[1])], wo[slot(order[1]), :])
    phase('wait_proj')
    landed(wo.at[rest], wo_sem.at[2])
    arrived(og.at[:, rest], a2a_recv.at[2])
    phase('proj_rest')
    for i, part in enumerate(spans):
        pp[:, part] += tall_dot(og[:, 2 * q_cols:], wo[2 * q_cols:, part])
        send(pp.at[:, part], precv.at[:, part], pp_send.at[0], pp_recv.at[i], mate)
    for j in range(n_col):
        load(wd_hbm.at[:, :, cols(core * half + j * COL, COL)], wa.at[:, :, j * COL:(j + 1) * COL], wd_sem.at[0])

    phase('wait_mate')
    dev_rows = pl.ds(pl.multiple_of(dev * rows, rows), rows)
    for i, part in enumerate(spans):
        arrived(precv.at[:, part], pp_recv.at[i])
        x1b[:, part] = (xres[:, part].astype(F32) + (pp[:, part] + precv[:, part])).astype(BF16)
    phase('norm2')
    inv2 = rms_scale(square_sums([x1b[:, i * COL:(i + 1) * COL].astype(F32) for i in range(2 * n_col)]), width)
    for i in range(2 * n_col):
        part = slice(i * COL, (i + 1) * COL)
        hg[dev_rows, part] = (x1b[:, part].astype(F32) * inv2 * fgain[:, part]).astype(BF16)

    phase('gather')
    ka = kq * pcol // 2
    kb = (half - kq * pcol) // 2
    strips = (((0, ka), (ka, ka)), ((2 * ka, kb), (2 * ka + kb, kb)))

    def piece(owner, strip, whose):
        owner_rows = pl.ds(pl.multiple_of(lax.rem(owner + 2 * n_dev, n_dev) * rows, rows), rows)
        return hg.at[owner_rows, cols(whose * half + strip[0], strip[1])]

    def across(step):
        return {**on_y(step), **mate}

    kind = (0, 1, 2, 2, 3, 3) + (4,) * 6

    def hop(owner, strip, p, i, where, whose):
        ref = piece(owner, strip, whose)
        send(ref, ref, ag_send.at[0], ag_recv.at[p, kind[i]], where)

    source = ((-1, 0), (1, 1), (-1, 1), (1, 0), (2, 0), (2, 1))
    def hop_own(p, late):
        if late:
            hop(dev, strips[p][1], p, 2, across(1), core)
            hop(dev, strips[p][0], p, 3, across(-1), core)
        else:
            hop(dev, strips[p][0], p, 0, across(1), core)
            hop(dev, strips[p][1], p, 1, across(-1), core)

    hop_own(0, False)
    hop_own(0, True)
    hop_own(1, False)

    def take_near(p, i):
        owner = dev + 2 * i - 1
        start = strips[p][0][0] + i * strips[p][0][1]
        ref = piece(owner, (start, strips[p][0][1]), 1 - core)
        arrived(ref, ag_recv.at[p, i])
        send(ref, ref, ag_send.at[0], ag_recv.at[p, 3], across(1 - 2 * i))
        send(ref, ref, ag_send.at[0], ag_recv.at[p, 4], mate)

    def both(p, count):
        return hg.at[0:rows, 0:count * strips[p][0][1]]

    def take_pair(p, first):
        arrived(both(p, 2), ag_recv.at[p, kind[first]])
        for i in (first, first + 1):
            owner, strip = dev + source[i][0], strips[p][source[i][1]]
            hop(owner, strip, p, 6 + i, mate, 1 - core if i < 4 else core)

    def from_mate(p):
        arrived(both(p, 6), ag_recv.at[p, 4])

    def weights(m, j, i):
        first, count = seg[i]
        main, tail = (wg, kbuf) if m == 0 else (wu, vbuf)
        if isinstance(j, int) and j >= n_main:
            start = (j - n_main) * prow + first
            return tail[start:start + count].reshape(count * pcol, COL)
        return main[first:first + count, :, cols(j * COL, COL)].reshape(count * pcol, COL)

    def partial_sum(m, j, p):
        out = None
        for i in (2 * p, 2 * p + 1):
            first, count = seg[i]
            term = dot(hg[:, first * pcol:(first + count) * pcol], weights(m, j, i))
            out = term if out is None else out + term
        return out

    def gate_up(p, group):
        for j in group:
            gate, up = partial_sum(0, j, p), partial_sum(1, j, p)
            if p == 0:
                yb[j] = gate
                ub[j] = up
            else:
                gate = yb[j] + gate
                gate = 0.5 * gate * (1.0 + jnp.tanh(0.5 * gate))
                u[:, cols(core * half + j * COL, COL)] = (gate * (ub[j] + up)).astype(BF16)
        if p == 1:
            for j in group:
                here = u.at[:, cols(core * half + j * COL, COL)]
                send(here, here, u_send.at[0], u_recv.at[0], mate)

    def gate_up_part(p):
        count = seg[2 * p][1]
        for m, (w_buf, tail) in enumerate(((wg, kbuf), (wu, vbuf))):
            landed(w_buf.at[pl.ds(0, 2 * count)], gu_sem.at[m, p])
            landed(tail.at[pl.ds(0, 2 * n_tail * count)], tail_sem.at[m, p])
        phase('gateup%d' % p)

        if p == 0:
            gate_up(p, range(n_col - 4))
            phase('gather2')
            take_pair(1, 2)
            take_pair(1, 4)
            phase('gateup0b')
            gate_up(p, range(n_col - 4, n_col))
        else:
            gate_up(p, range(n_col - 3))
            gate_up(p, range(n_col - 3, n_col - 1))
            gate_up(p, range(n_col - 1, n_col))

    near = 1 - jnp.minimum(dev, 1)
    take_near(0, near)
    take_near(0, 1 - near)
    hop_own(1, True)
    phase('gather_b')
    take_pair(0, 2)
    take_near(1, near)
    take_near(1, 1 - near)
    phase('gather_c')
    take_pair(0, 4)
    from_mate(0)
    phase('wait_gu0')
    gate_up_part(0)
    phase('gather3')
    from_mate(1)
    phase('wait_gu1')
    gate_up_part(1)
    phase('down0')
    fold_half = half // pcol

    def down_half(whose, group):
        at = pl.ds(whose * fold_half, fold_half)
        part = slice(group[0] * COL, (group[-1] + 1) * COL)
        return dot(u[:, cols(whose * half, half)], wa[at, :, part].reshape(half, len(group) * COL))

    def keep(group, value, add):
        for n, j in enumerate(group):
            piece_of = value[:, n * COL:(n + 1) * COL]
            yb[j] = yb[j] + piece_of if add else piece_of

    pairs = [range(j, min(j + 2, n_col)) for j in range(0, n_col, 2)]
    landed(wa, wd_sem.at[0])
    for group in pairs[:2]:
        keep(group, down_half(core, group), False)

    phase('wait_u')
    arrived(u.at[:, cols((1 - core) * half, half)], u_recv.at[0])

    phase('down')
    def way(j):
        sign = (1 - 2 * core) * (1 - 2 * (j % 2))
        return sign

    def rows_of(owner):
        return pl.ds(pl.multiple_of(lax.rem(owner + 2 * n_dev, n_dev) * rows, rows), rows)

    blk = rows // CORES
    sides = [{'side': CORES * chip + b} for b in range(CORES)]

    def block_of(owner, b):
        start = lax.rem(owner + 2 * n_dev, n_dev) * rows + b * blk
        return pl.ds(pl.multiple_of(start, blk), blk)

    def pass_far(j):
        send(yb.at[j, rows_of(dev + 2)], r1.at[j], rs_send.at[0], far_recv.at[j], on_y(way(j)))

    def pass_near(j):
        sign = way(j)
        for b in range(CORES):
            send(yb.at[j, block_of(dev - sign, b)], r3.at[core, j], rs_send.at[2], rs_recv.at[1],
                 {**on_y(-sign), **sides[b]})

    def pass_sum(j):
        sign = way(j)
        arrived(r1.at[j], far_recv.at[j])
        yb[j, rows_of(dev + sign), :] += r1[j]
        for b in range(CORES):
            send(yb.at[j, block_of(dev + sign, b)], r2.at[core, j], rs_send.at[1], rs_recv.at[0],
                 {**on_y(sign), **sides[b]})

    for group in pairs:
        if group in pairs[:2]:
            keep(group, down_half(1 - core, group), True)
        else:
            part = slice(group[0] * COL, (group[-1] + 1) * COL)
            keep(group, dot(u[...], wa[:, :, part].reshape(prow * pcol, len(group) * COL)), False)
        for j in group:
            pass_far(j)

    phase('stage2')
    for j in range(n_col):
        pass_near(j)
    for j in range(n_col):
        send(yb.at[j, block_of(dev, 1 - core)], r4.at[j], fin_send.at[0], fin_recv.at[0], mate)
    for j in range(n_col):
        pass_sum(j)

    phase('final')
    my_blk = pl.ds(pl.multiple_of(core * blk, blk), blk)

    def finish(whose, j, own_sum):
        y = (own_sum + r2[whose, j] + r3[whose, j]).astype(BF16)
        here = cols(whose * half + j * COL, COL)
        out[:, here] = (x1b[my_blk, here].astype(F32) + y.astype(F32)).astype(BF16)

    arrived(r4, fin_recv.at[0])
    arrived(r3, rs_recv.at[1])
    arrived(r2, rs_recv.at[0])
    for j in range(n_col):
        finish(core, j, yb[j, block_of(dev, core), :])
        finish(1 - core, j, r4[j])
    phase('drain')
    arrived(og.at[:, q_cols:], a2a_send.at[0])
    arrived(pp, pp_send.at[0])
    arrived(hg.at[0:(CORES + 1) * rows], ag_send.at[0])
    arrived(u.at[:, cols(core * half, half)], u_send.at[0])
    arrived(r1, rs_send.at[0])
    arrived(r2, rs_send.at[1])
    arrived(r3, rs_send.at[2])
    arrived(r4, fin_send.at[0])
    phase(None)


def solution(mesh):
    n_side = mesh.shape['side']
    n_dev = mesh.shape['dev']
    batch_axes = ('inst', 'dev')
    in_specs = (
        P(batch_axes, None),
        P(batch_axes),
        P(None, batch_axes, None, None, None),
        P(None, batch_axes, None, None, None),
        P(), P(), P(), P(), P(),
        P(None, None, 'dev'),
        P(None, None, 'dev'),
        P(None, 'dev', None),
    )
    out_specs = P(('inst', 'dev', 'side'), None)

    def device_fn(hidden, cache_len, k_cache, v_cache, w_q, w_kv, w_o, attn_gain, ffn_gain, w_gate, w_up, w_down):
        seqs, width = hidden.shape
        span, head = k_cache.shape[3:]
        ff = w_gate.shape[2]
        half = width // 2
        rows = seqs * CORES // n_side
        n_x = n_side // CORES
        n_col = half // COL
        q_cols = w_q.shape[2] // n_side
        tall = width // span
        freqs = jnp.asarray(ROPE_BASE ** (-np.arange(head // 2, dtype=np.float64) / (head // 2)), F32)[None]

        def fold(w):
            return w.reshape(w.shape[1] // span, span, w.shape[2])

        args = (hidden, cache_len.reshape(1, seqs), freqs, k_cache[0], v_cache[0], fold(w_q), fold(w_kv),
                w_o.reshape(n_side, w_o.shape[1] // n_side, width), attn_gain, ffn_gain,
                fold(w_gate), fold(w_up), fold(w_down))
        vmem = pltpu.VMEM
        dma = pltpu.SemaphoreType.DMA
        main = ff // CORES - 2 * COL
        scratch = [
            vmem((seqs, width), BF16), vmem((1, seqs), jnp.int32), vmem((1, head // 2), F32),
            vmem((1, width), F32), vmem((1, width), F32), vmem((rows, width), BF16),
            vmem((tall, span, half), BF16),
            vmem((seqs, span, head), BF16), vmem((seqs, span, head), BF16),
            vmem((n_x * q_cols, width), BF16),
            vmem((tall, span, main), BF16), vmem((tall, span, main), BF16),
            vmem((n_col, seqs, COL), F32), vmem((n_col, seqs, COL), F32), vmem((seqs, 1), F32),
            vmem((seqs, q_cols), BF16), vmem((rows, n_x * q_cols), BF16),
            vmem((rows, width), F32), vmem((rows, width), F32), vmem((rows, width), BF16),
            vmem((n_dev * rows, width), BF16), vmem((seqs, ff), BF16),
            vmem((n_col, rows, COL), F32), vmem((CORES, n_col, rows // CORES, COL), F32),
            vmem((CORES, n_col, rows // CORES, COL), F32), vmem((n_col, rows // CORES, COL), F32),
            dma((6,)), dma((4,)), dma((3,)), dma((3,)), dma((2, 2)), dma((2, 2)), dma((1,)),
            dma((1,)), dma((3,)), dma((1,)), dma((2,)), dma((1,)), dma((2, 5)), dma((1,)), dma((1,)),
            dma((3,)), dma((2,)), dma((n_col,)), dma((1,)), dma((1,)),
        ]
        anywhere = pl.BlockSpec(memory_space=pl.ANY)
        return pl.pallas_call(
            functools.partial(layer_kernel, n_dev, n_side),
            out_shape=jax.ShapeDtypeStruct((rows // CORES, width), BF16),
            in_specs=[anywhere] * len(args),
            out_specs=pl.BlockSpec(memory_space=pltpu.VMEM),
            scratch_shapes=scratch,
            compiler_params=pltpu.CompilerParams(
                collective_id=0, has_side_effects=True, vmem_limit_bytes=67_043_328),
        )(*args)

    return jax.shard_map(device_fn, mesh=mesh, in_specs=in_specs, out_specs=out_specs, check_vma=False)
```

```python
import functools

import jax
import jax.numpy as jnp
import numpy as np
from jax import lax
from jax.experimental import pallas as pl
from jax.experimental.pallas import tpu as pltpu
from jax.sharding import PartitionSpec as P

EPS = 1e-5
ROPE_BASE = 10000.0
MESH = pl.DeviceIdType.MESH
F32 = jnp.float32
BF16 = jnp.bfloat16
COL = 256
CORES = 2
NEG = -1e30


def dot(lhs, rhs):
    return jnp.dot(lhs, rhs, preferred_element_type=F32)


def rms_scale(square_sum, width):
    return lax.rsqrt(square_sum / width + EPS)


def square_sums(parts):
    acc = None
    for part in parts:
        for g in range(part.shape[1] // 128):
            x = part[:, g * 128:(g + 1) * 128]
            acc = x * x if acc is None else acc + x * x
    return jnp.sum(acc, axis=1, keepdims=True)


def pair_blocks(first, second):
    rows, n = first.shape
    both = jnp.concatenate([first.reshape(rows // 8, 8, n), second.reshape(rows // 8, 8, n)], axis=1)
    return both.reshape(2 * rows, n)


class Phases:
    def __init__(self):
        self.scope = None

    def __call__(self, name):
        if self.scope is not None:
            self.scope.__exit__(None, None, None)
        self.scope = None if name is None else jax.named_scope(name)
        if self.scope is not None:
            self.scope.__enter__()


def layer_kernel(n_dev, n_side,
                 x_hbm, len_hbm, freq_hbm, k_hbm, v_hbm, wq_hbm, wkv_hbm, wo_hbm, again_hbm, fgain_hbm,
                 wg_hbm, wu_hbm, wd_hbm, out,
                 act, lens, freqs, again, fgain, xres, wa, kbuf, vbuf, wo, wg, wu,
                 yb, ub, lenc, osend, og, pp, precv, x1b, hg, u, r1, r2, r3, r4,
                 in_sem, w_sem, kv_sem, wo_sem, gu_sem, tail_sem, wd_sem,
                 a2a_send, a2a_recv, pp_send, pp_recv, ag_send, ag_recv, u_send, u_recv,
                 rs_send, rs_recv, far_recv, fin_send, fin_recv):
    dev = lax.axis_index('dev')
    side = lax.axis_index('side')
    n_x = n_side // CORES
    chip = lax.div(side, CORES)
    core = lax.rem(side, CORES)
    mate = {'side': CORES * chip + 1 - core}
    seqs, width = act.shape
    head = COL
    q_cols = osend.shape[1]
    half = width // 2
    rows = xres.shape[0]
    n_col = half // COL
    kq = (n_col + 1) // 2 * COL // wa.shape[1]
    n_main = wg.shape[2] // COL
    n_tail = n_col - n_main
    kv_half = wkv_hbm.shape[2] // 2
    prow, pcol = wa.shape[0], wa.shape[1]

    def on_x(r):
        return {'side': CORES * lax.rem(chip + r, n_x) + 1 - core}

    def on_y(r):
        return {'dev': lax.rem(dev + r + n_dev, n_dev)}

    phase = Phases()
    phase('start')
    barrier = pltpu.get_barrier_semaphore()
    peers = [mate] + [on_x(r) for r in range(1, n_x)] + [on_y(1), on_y(-1)]
    peers += [{**on_y(1), **mate}, {**on_y(-1), **mate}]
    for peer in peers:
        pl.semaphore_signal(barrier, inc=1, device_id=peer, device_id_type=MESH)

    def cols(start, size):
        return pl.ds(pl.multiple_of(start, 128), size)

    def load(src, dst, sem, priority=1):
        pltpu.make_async_copy(src, dst, sem).start(priority=priority)

    def landed(dst, sem):
        pltpu.make_async_copy(dst, dst, sem).wait()

    cut = (n_col + 1) // 2 * 2 * COL
    spans = (slice(0, cut), slice(cut, width))
    my_rows = pl.ds(pl.multiple_of(chip * rows, rows), rows)

    load(x_hbm, act, in_sem.at[0], 0)
    load(len_hbm, lens, in_sem.at[1], 0)
    load(freq_hbm, freqs, in_sem.at[2], 0)
    load(again_hbm, again, in_sem.at[3], 0)
    load(fgain_hbm, fgain, in_sem.at[4], 0)
    load(x_hbm.at[my_rows], xres, in_sem.at[5], 0)

    def w_slot(j):
        return wa.at[:, :, j * COL:(j + 1) * COL]

    load(wq_hbm.at[:, :, cols(side * q_cols, COL)], w_slot(0), w_sem.at[0])
    load(wq_hbm.at[:, :, cols(side * q_cols + COL, COL)], w_slot(1), w_sem.at[1])
    load(wkv_hbm.at[:, :, cols(side * head, COL)], w_slot(2), w_sem.at[2])
    load(wkv_hbm.at[:, :, cols(kv_half + side * head, COL)], w_slot(3), w_sem.at[3])
    phase('wait_x')
    for i, ref in enumerate((act, lens, freqs, again, fgain, xres)):
        landed(ref, in_sem.at[i])
    by_distance = sorted(range(1, n_x), key=lambda r: (-min(r, n_x - r), r)) + [0]

    def cache_rows(r):
        return pl.ds(lax.rem(chip + r, n_x) * rows, rows)

    def load_cache(r):
        at = cache_rows(r)
        group = by_distance.index(r)
        load(k_hbm.at[at, side], kbuf.at[at], kv_sem.at[group])
        load(v_hbm.at[at, side], vbuf.at[at], kv_sem.at[group])

    order = [0] + by_distance[:-1]

    def slot(r):
        start = order.index(r) * q_cols
        return slice(start, start + q_cols)

    def wo_slot(r):
        return wo.at[slot(r)]

    def load_wo(r):
        src_core = core if r == 0 else 1 - core
        load(wo_hbm.at[CORES * lax.rem(chip + n_x - r, n_x) + src_core], wo_slot(r), wo_sem.at[min(order.index(r), 2)])

    load_cache(by_distance[0])
    phase('tables')
    row_id = lax.broadcasted_iota(jnp.int32, (seqs, seqs), 0)
    col_id = lax.broadcasted_iota(jnp.int32, (seqs, seqs), 1)
    wide = jnp.broadcast_to(lens[...].astype(F32), (seqs, seqs))
    len_col = jnp.sum(jnp.where(row_id == col_id, wide, 0.0), axis=1, keepdims=True)
    angle = len_col * freqs[...]
    cos_part = jnp.cos(angle)
    sin_part = jnp.sin(angle)

    def rotate(vecs):
        first, second = vecs[:, :head // 2], vecs[:, head // 2:]
        return jnp.concatenate([first * cos_part - second * sin_part, second * cos_part + first * sin_part], axis=1)

    phase('norm1')
    inv = rms_scale(square_sums([act[:, i * COL:(i + 1) * COL].astype(F32) for i in range(2 * n_col)]), width)
    for i in range(2 * n_col):
        part = slice(i * COL, (i + 1) * COL)
        act[:, part] = (act[:, part].astype(F32) * inv * again[:, part]).astype(BF16)

    phase('qkv')
    lenc[...] = len_col

    for j in range(4):
        landed(w_slot(0), w_sem.at[j])
        if j:
            load_cache(by_distance[j])
        yb[j] = dot(act[...], wa[:, :, cols(j * COL, COL)].reshape(prow * pcol, COL))

    load_wo(0)
    load_wo(order[1])
    phase('rope')
    for j in range(4):
        vecs = yb[j] if j == 3 else rotate(yb[j])
        yb[j] = vecs.astype(BF16).astype(F32)

    span = kbuf.shape[1]
    keys = 8 * span
    scale = head ** -0.5
    groups = rows // 8
    row = lax.broadcasted_iota(jnp.int32, (2 * rows, keys), 0)
    key = lax.broadcasted_iota(jnp.int32, (2 * rows, keys), 1)
    offset = key - lax.rem(row, 8) * span

    def cat(parts):
        return parts[0] if len(parts) == 1 else jnp.concatenate(parts, axis=0)

    def attend(theres):
        ats = [pl.ds(pl.multiple_of(there * rows, rows), rows) for there in theres]
        q0, q1, k_new, v_new = (cat([yb[j, at, :] for at in ats]) for j in range(4))
        q_pair = pair_blocks(q0, q1).astype(BF16)
        self_score = pair_blocks(jnp.sum(q0 * k_new, axis=1, keepdims=True),
                                 jnp.sum(q1 * k_new, axis=1, keepdims=True)) * scale
        lengths = cat([lenc[at, :] for at in ats])
        len_rows = pair_blocks(lengths, lengths).astype(jnp.int32)
        blocks = [there * rows + 8 * b for there in theres for b in range(groups)]
        scores = cat([
            lax.dot_general(q_pair[16 * n:16 * n + 16], kbuf[pl.ds(b, 8)].reshape(keys, head),
                            (((1,), (1,)), ((), ())), preferred_element_type=F32)
            for n, b in enumerate(blocks)])
        offsets = cat([offset] * len(theres))
        scores = jnp.where((offsets >= 0) & (offsets < len_rows), scores * scale, NEG)
        row_max = jnp.maximum(jnp.max(scores, axis=1, keepdims=True), self_score)
        exp_scores = jnp.exp(scores - row_max)
        self_exp = jnp.exp(self_score - row_max)
        total = jnp.sum(exp_scores, axis=1, keepdims=True) + self_exp
        probs = exp_scores.astype(BF16)
        mixed = cat([dot(probs[16 * n:16 * n + 16], vbuf[pl.ds(b, 8)].reshape(keys, head))
                     for n, b in enumerate(blocks)])
        mixed = mixed + self_exp.astype(BF16).astype(F32) * pair_blocks(v_new, v_new)
        mixed = (mixed / total).reshape(len(blocks), 16, head)
        first = mixed[:, :8].reshape(len(theres) * rows, head).astype(BF16)
        second = mixed[:, 8:].reshape(len(theres) * rows, head).astype(BF16)
        for n, at in enumerate(ats):
            osend[at, :head] = first[n * rows:(n + 1) * rows]
            osend[at, head:] = second[n * rows:(n + 1) * rows]
        return ats

    def send(src, dst, send_sem, recv_sem, where):
        pltpu.make_async_remote_copy(src, dst, send_sem, recv_sem, device_id=where, device_id_type=MESH).start()

    def arrived(dst, sem):
        pltpu.make_async_copy(dst, dst, sem).wait()

    def og_slot(r):
        return og.at[:, slot(r)]

    pl.semaphore_wait(barrier, len(peers))
    for group, pair in enumerate([[r] for r in by_distance]):
        phase('wait_kv%d' % pair[0])
        landed(kbuf.at[pl.ds(0, 2 * len(pair) * rows)], kv_sem.at[group])
        phase('attend%d' % pair[0])
        ats = attend([lax.rem(chip + r, n_x) for r in pair])
        for r, at in zip(pair, ats):
            if r:
                send(osend.at[at], og_slot(r), a2a_send.at[0], a2a_recv.at[min(order.index(r), 2)], on_x(r))
        if pair[0] == by_distance[0]:
            for other in order[2:]:
                load_wo(other)

    phase('loads2')
    seg = ((0, kq), (half // pcol, kq), (kq, half // pcol - kq), (half // pcol + kq, half // pcol - kq))

    def load_gate_up(part):
        for i in (2 * part, 2 * part + 1):
            first, count = seg[i]
            at = pl.ds(first, count)
            for m, (w_hbm, w_buf, tail) in enumerate(((wg_hbm, wg, kbuf), (wu_hbm, wu, vbuf))):
                load(w_hbm.at[at, :, cols(core * half, n_main * COL)], w_buf.at[at], gu_sem.at[m, part])
                for t in range(n_tail):
                    load(w_hbm.at[at, :, cols(core * half + (n_main + t) * COL, COL)],
                         tail.at[pl.ds(t * prow + first, count)], tail_sem.at[m, part])

    load_gate_up(0)
    load_gate_up(1)
    phase('proj')
    def tall_dot(lhs, rhs):
        return dot(jnp.concatenate([lhs] * 4, axis=0), rhs)[:rows]

    phase('proj0')
    landed(wo_slot(0), wo_sem.at[0])
    pp[...] = dot(osend[my_rows, :], wo[0:q_cols, :])
    rest = slice(2 * q_cols, n_x * q_cols)
    phase('proj1')
    landed(wo_slot(order[1]), wo_sem.at[1])
    arrived(og_slot(order[1]), a2a_recv.at[1])
    pp[...] += tall_dot(og[:, slot(order[1])], wo[slot(order[1]), :])
    phase('wait_proj')
    landed(wo.at[rest], wo_sem.at[2])
    arrived(og.at[:, rest], a2a_recv.at[2])
    phase('proj_rest')
    for i, part in enumerate(spans):
        pp[:, part] += tall_dot(og[:, 2 * q_cols:], wo[2 * q_cols:, part])
        send(pp.at[:, part], precv.at[:, part], pp_send.at[0], pp_recv.at[i], mate)
    for j in range(n_col):
        load(wd_hbm.at[:, :, cols(core * half + j * COL, COL)], wa.at[:, :, j * COL:(j + 1) * COL], wd_sem.at[0])

    phase('wait_mate')
    dev_rows = pl.ds(pl.multiple_of(dev * rows, rows), rows)
    for i, part in enumerate(spans):
        arrived(precv.at[:, part], pp_recv.at[i])
        x1b[:, part] = (xres[:, part].astype(F32) + (pp[:, part] + precv[:, part])).astype(BF16)
    phase('norm2')
    inv2 = rms_scale(square_sums([x1b[:, i * COL:(i + 1) * COL].astype(F32) for i in range(2 * n_col)]), width)
    for i in range(2 * n_col):
        part = slice(i * COL, (i + 1) * COL)
        hg[dev_rows, part] = (x1b[:, part].astype(F32) * inv2 * fgain[:, part]).astype(BF16)

    phase('gather')
    ka = kq * pcol // 2
    kb = (half - kq * pcol) // 2
    strips = (((0, ka), (ka, ka)), ((2 * ka, kb), (2 * ka + kb, kb)))

    def piece(owner, strip, whose):
        owner_rows = pl.ds(pl.multiple_of(lax.rem(owner + 2 * n_dev, n_dev) * rows, rows), rows)
        return hg.at[owner_rows, cols(whose * half + strip[0], strip[1])]

    def across(step):
        return {**on_y(step), **mate}

    kind = (0, 1, 2, 2, 3, 3) + (4,) * 6

    def hop(owner, strip, p, i, where, whose):
        ref = piece(owner, strip, whose)
        send(ref, ref, ag_send.at[0], ag_recv.at[p, kind[i]], where)

    source = ((-1, 0), (1, 1), (-1, 1), (1, 0), (2, 0), (2, 1))
    def hop_own(p, late):
        if late:
            hop(dev, strips[p][1], p, 2, across(1), core)
            hop(dev, strips[p][0], p, 3, across(-1), core)
        else:
            hop(dev, strips[p][0], p, 0, across(1), core)
            hop(dev, strips[p][1], p, 1, across(-1), core)

    hop_own(0, False)
    hop_own(0, True)
    hop_own(1, False)

    def take_near(p, i):
        owner = dev + 2 * i - 1
        start = strips[p][0][0] + i * strips[p][0][1]
        ref = piece(owner, (start, strips[p][0][1]), 1 - core)
        arrived(ref, ag_recv.at[p, i])
        send(ref, ref, ag_send.at[0], ag_recv.at[p, 3], across(1 - 2 * i))
        send(ref, ref, ag_send.at[0], ag_recv.at[p, 4], mate)

    def both(p, count):
        return hg.at[0:rows, 0:count * strips[p][0][1]]

    def take_pair(p, first):
        arrived(both(p, 2), ag_recv.at[p, kind[first]])
        for i in (first, first + 1):
            owner, strip = dev + source[i][0], strips[p][source[i][1]]
            hop(owner, strip, p, 6 + i, mate, 1 - core if i < 4 else core)

    def from_mate(p):
        arrived(both(p, 6), ag_recv.at[p, 4])

    def weights(m, j, i):
        first, count = seg[i]
        main, tail = (wg, kbuf) if m == 0 else (wu, vbuf)
        if isinstance(j, int) and j >= n_main:
            start = (j - n_main) * prow + first
            return tail[start:start + count].reshape(count * pcol, COL)
        return main[first:first + count, :, cols(j * COL, COL)].reshape(count * pcol, COL)

    def partial_sum(m, j, p):
        out = None
        for i in (2 * p, 2 * p + 1):
            first, count = seg[i]
            term = dot(hg[:, first * pcol:(first + count) * pcol], weights(m, j, i))
            out = term if out is None else out + term
        return out

    def gate_up(p, group):
        for j in group:
            gate, up = partial_sum(0, j, p), partial_sum(1, j, p)
            if p == 0:
                yb[j] = gate
                ub[j] = up
            else:
                gate = yb[j] + gate
                gate = 0.5 * gate * (1.0 + jnp.tanh(0.5 * gate))
                u[:, cols(core * half + j * COL, COL)] = (gate * (ub[j] + up)).astype(BF16)
        if p == 1:
            for j in group:
                here = u.at[:, cols(core * half + j * COL, COL)]
                send(here, here, u_send.at[0], u_recv.at[0], mate)

    def gate_up_part(p):
        count = seg[2 * p][1]
        for m, (w_buf, tail) in enumerate(((wg, kbuf), (wu, vbuf))):
            landed(w_buf.at[pl.ds(0, 2 * count)], gu_sem.at[m, p])
            landed(tail.at[pl.ds(0, 2 * n_tail * count)], tail_sem.at[m, p])
        phase('gateup%d' % p)

        if p == 0:
            gate_up(p, range(n_col - 4))
            phase('gather2')
            take_pair(1, 2)
            take_pair(1, 4)
            phase('gateup0b')
            gate_up(p, range(n_col - 4, n_col))
        else:
            gate_up(p, range(n_col - 2))
            gate_up(p, range(n_col - 2, n_col))

    near = 1 - jnp.minimum(dev, 1)
    take_near(0, near)
    take_near(0, 1 - near)
    hop_own(1, True)
    phase('gather_b')
    take_pair(0, 2)
    take_near(1, near)
    take_near(1, 1 - near)
    phase('gather_c')
    take_pair(0, 4)
    from_mate(0)
    phase('wait_gu0')
    gate_up_part(0)
    phase('gather3')
    from_mate(1)
    phase('wait_gu1')
    gate_up_part(1)
    phase('down0')
    fold_half = half // pcol

    def down_half(whose, group):
        at = pl.ds(whose * fold_half, fold_half)
        part = slice(group[0] * COL, (group[-1] + 1) * COL)
        return dot(u[:, cols(whose * half, half)], wa[at, :, part].reshape(half, len(group) * COL))

    def keep(group, value, add):
        for n, j in enumerate(group):
            piece_of = value[:, n * COL:(n + 1) * COL]
            yb[j] = yb[j] + piece_of if add else piece_of

    pairs = [range(j, min(j + 2, n_col)) for j in range(0, n_col, 2)]
    landed(wa, wd_sem.at[0])
    for group in pairs[:2]:
        keep(group, down_half(core, group), False)

    phase('wait_u')
    arrived(u.at[:, cols((1 - core) * half, half)], u_recv.at[0])

    phase('down')
    def way(j):
        sign = (1 - 2 * core) * (1 - 2 * (j % 2))
        return sign

    def rows_of(owner):
        return pl.ds(pl.multiple_of(lax.rem(owner + 2 * n_dev, n_dev) * rows, rows), rows)

    blk = rows // CORES
    sides = [{'side': CORES * chip + b} for b in range(CORES)]

    def block_of(owner, b):
        start = lax.rem(owner + 2 * n_dev, n_dev) * rows + b * blk
        return pl.ds(pl.multiple_of(start, blk), blk)

    def pass_far(j):
        send(yb.at[j, rows_of(dev + 2)], r1.at[j], rs_send.at[0], far_recv.at[j], on_y(way(j)))

    def pass_near(j):
        sign = way(j)
        for b in range(CORES):
            send(yb.at[j, block_of(dev - sign, b)], r3.at[core, j], rs_send.at[2], rs_recv.at[1],
                 {**on_y(-sign), **sides[b]})

    def pass_sum(j):
        sign = way(j)
        arrived(r1.at[j], far_recv.at[j])
        yb[j, rows_of(dev + sign), :] += r1[j]
        for b in range(CORES):
            send(yb.at[j, block_of(dev + sign, b)], r2.at[core, j], rs_send.at[1], rs_recv.at[0],
                 {**on_y(sign), **sides[b]})

    for group in pairs:
        if group in pairs[:2]:
            keep(group, down_half(1 - core, group), True)
        else:
            part = slice(group[0] * COL, (group[-1] + 1) * COL)
            keep(group, dot(u[...], wa[:, :, part].reshape(prow * pcol, len(group) * COL)), False)
        for j in group:
            pass_far(j)

    phase('stage2')
    for j in range(n_col):
        pass_near(j)
    for j in range(n_col):
        send(yb.at[j, block_of(dev, 1 - core)], r4.at[j], fin_send.at[0], fin_recv.at[0], mate)
    for j in range(n_col):
        pass_sum(j)

    phase('final')
    my_blk = pl.ds(pl.multiple_of(core * blk, blk), blk)

    def finish(whose, j, own_sum):
        y = (own_sum + r2[whose, j] + r3[whose, j]).astype(BF16)
        here = cols(whose * half + j * COL, COL)
        out[:, here] = (x1b[my_blk, here].astype(F32) + y.astype(F32)).astype(BF16)

    arrived(r4, fin_recv.at[0])
    arrived(r3, rs_recv.at[1])
    arrived(r2, rs_recv.at[0])
    for j in range(n_col):
        finish(core, j, yb[j, block_of(dev, core), :])
        finish(1 - core, j, r4[j])
    phase('drain')
    arrived(og.at[:, q_cols:], a2a_send.at[0])
    arrived(pp, pp_send.at[0])
    arrived(hg.at[0:(CORES + 1) * rows], ag_send.at[0])
    arrived(u.at[:, cols(core * half, half)], u_send.at[0])
    arrived(r1, rs_send.at[0])
    arrived(r2, rs_send.at[1])
    arrived(r3, rs_send.at[2])
    arrived(r4, fin_send.at[0])
    phase(None)


def solution(mesh):
    n_side = mesh.shape['side']
    n_dev = mesh.shape['dev']
    batch_axes = ('inst', 'dev')
    in_specs = (
        P(batch_axes, None),
        P(batch_axes),
        P(None, batch_axes, None, None, None),
        P(None, batch_axes, None, None, None),
        P(), P(), P(), P(), P(),
        P(None, None, 'dev'),
        P(None, None, 'dev'),
        P(None, 'dev', None),
    )
    out_specs = P(('inst', 'dev', 'side'), None)

    def device_fn(hidden, cache_len, k_cache, v_cache, w_q, w_kv, w_o, attn_gain, ffn_gain, w_gate, w_up, w_down):
        seqs, width = hidden.shape
        span, head = k_cache.shape[3:]
        ff = w_gate.shape[2]
        half = width // 2
        rows = seqs * CORES // n_side
        n_x = n_side // CORES
        n_col = half // COL
        q_cols = w_q.shape[2] // n_side
        tall = width // span
        freqs = jnp.asarray(ROPE_BASE ** (-np.arange(head // 2, dtype=np.float64) / (head // 2)), F32)[None]

        def fold(w):
            return w.reshape(w.shape[1] // span, span, w.shape[2])

        args = (hidden, cache_len.reshape(1, seqs), freqs, k_cache[0], v_cache[0], fold(w_q), fold(w_kv),
                w_o.reshape(n_side, w_o.shape[1] // n_side, width), attn_gain, ffn_gain,
                fold(w_gate), fold(w_up), fold(w_down))
        vmem = pltpu.VMEM
        dma = pltpu.SemaphoreType.DMA
        main = ff // CORES - 2 * COL
        scratch = [
            vmem((seqs, width), BF16), vmem((1, seqs), jnp.int32), vmem((1, head // 2), F32),
            vmem((1, width), F32), vmem((1, width), F32), vmem((rows, width), BF16),
            vmem((tall, span, half), BF16),
            vmem((seqs, span, head), BF16), vmem((seqs, span, head), BF16),
            vmem((n_x * q_cols, width), BF16),
            vmem((tall, span, main), BF16), vmem((tall, span, main), BF16),
            vmem((n_col, seqs, COL), F32), vmem((n_col, seqs, COL), F32), vmem((seqs, 1), F32),
            vmem((seqs, q_cols), BF16), vmem((rows, n_x * q_cols), BF16),
            vmem((rows, width), F32), vmem((rows, width), F32), vmem((rows, width), BF16),
            vmem((n_dev * rows, width), BF16), vmem((seqs, ff), BF16),
            vmem((n_col, rows, COL), F32), vmem((CORES, n_col, rows // CORES, COL), F32),
            vmem((CORES, n_col, rows // CORES, COL), F32), vmem((n_col, rows // CORES, COL), F32),
            dma((6,)), dma((4,)), dma((n_x,)), dma((3,)), dma((2, 2)), dma((2, 2)), dma((1,)),
            dma((1,)), dma((3,)), dma((1,)), dma((2,)), dma((1,)), dma((2, 5)), dma((1,)), dma((1,)),
            dma((3,)), dma((2,)), dma((n_col,)), dma((1,)), dma((1,)),
        ]
        anywhere = pl.BlockSpec(memory_space=pl.ANY)
        return pl.pallas_call(
            functools.partial(layer_kernel, n_dev, n_side),
            out_shape=jax.ShapeDtypeStruct((rows // CORES, width), BF16),
            in_specs=[anywhere] * len(args),
            out_specs=pl.BlockSpec(memory_space=pltpu.VMEM),
            scratch_shapes=scratch,
            compiler_params=pltpu.CompilerParams(
                collective_id=0, has_side_effects=True, vmem_limit_bytes=67_043_328),
        )(*args)

    return jax.shard_map(device_fn, mesh=mesh, in_specs=in_specs, out_specs=out_specs, check_vma=False)
```

```python
import functools

import jax
import jax.numpy as jnp
import numpy as np
from jax import lax
from jax.experimental import pallas as pl
from jax.experimental.pallas import tpu as pltpu
from jax.sharding import PartitionSpec as P

EPS = 1e-5
ROPE_BASE = 10000.0
MESH = pl.DeviceIdType.MESH
F32 = jnp.float32
BF16 = jnp.bfloat16
COL = 256
CORES = 2
NEG = -1e30


def dot(lhs, rhs):
    return jnp.dot(lhs, rhs, preferred_element_type=F32)


def rms_scale(square_sum, width):
    return lax.rsqrt(square_sum / width + EPS)


def square_sums(parts):
    acc = None
    for part in parts:
        for g in range(part.shape[1] // 128):
            x = part[:, g * 128:(g + 1) * 128]
            acc = x * x if acc is None else acc + x * x
    return jnp.sum(acc, axis=1, keepdims=True)


def pair_blocks(first, second):
    rows, n = first.shape
    both = jnp.concatenate([first.reshape(rows // 8, 8, n), second.reshape(rows // 8, 8, n)], axis=1)
    return both.reshape(2 * rows, n)


class Phases:
    def __init__(self):
        self.scope = None

    def __call__(self, name):
        if self.scope is not None:
            self.scope.__exit__(None, None, None)
        self.scope = None if name is None else jax.named_scope(name)
        if self.scope is not None:
            self.scope.__enter__()


def layer_kernel(n_dev, n_side,
                 x_hbm, len_hbm, freq_hbm, k_hbm, v_hbm, wq_hbm, wkv_hbm, wo_hbm, again_hbm, fgain_hbm,
                 wg_hbm, wu_hbm, wd_hbm, out,
                 act, lens, freqs, again, fgain, xres, wa, kbuf, vbuf, wo, wg, wu,
                 yb, ub, lenc, osend, og, pp, precv, x1b, hg, u, r1, r2, r3, r4,
                 in_sem, w_sem, kv_sem, wo_sem, gu_sem, tail_sem, wd_sem,
                 a2a_send, a2a_recv, pp_send, pp_recv, ag_send, ag_recv, u_send, u_recv,
                 rs_send, rs_recv, far_recv, fin_send, fin_recv):
    dev = lax.axis_index('dev')
    side = lax.axis_index('side')
    n_x = n_side // CORES
    chip = lax.div(side, CORES)
    core = lax.rem(side, CORES)
    mate = {'side': CORES * chip + 1 - core}
    seqs, width = act.shape
    head = COL
    q_cols = osend.shape[1]
    half = width // 2
    rows = xres.shape[0]
    n_col = half // COL
    kq = (n_col + 1) // 2 * COL // wa.shape[1]
    n_main = wg.shape[2] // COL
    n_tail = n_col - n_main
    kv_half = wkv_hbm.shape[2] // 2
    prow, pcol = wa.shape[0], wa.shape[1]

    def on_x(r):
        return {'side': CORES * lax.rem(chip + r, n_x) + 1 - core}

    def on_y(r):
        return {'dev': lax.rem(dev + r + n_dev, n_dev)}

    phase = Phases()
    phase('start')
    barrier = pltpu.get_barrier_semaphore()
    peers = [mate] + [on_x(r) for r in range(1, n_x)] + [on_y(1), on_y(-1)]
    peers += [{**on_y(1), **mate}, {**on_y(-1), **mate}]
    for peer in peers:
        pl.semaphore_signal(barrier, inc=1, device_id=peer, device_id_type=MESH)

    def cols(start, size):
        return pl.ds(pl.multiple_of(start, 128), size)

    def load(src, dst, sem, priority=1):
        pltpu.make_async_copy(src, dst, sem).start(priority=priority)

    def landed(dst, sem):
        pltpu.make_async_copy(dst, dst, sem).wait()

    cut = (n_col + 1) // 2 * 2 * COL
    spans = (slice(0, cut), slice(cut, width))
    my_rows = pl.ds(pl.multiple_of(chip * rows, rows), rows)

    load(x_hbm, act, in_sem.at[0], 0)
    load(len_hbm, lens, in_sem.at[1], 0)
    load(freq_hbm, freqs, in_sem.at[2], 0)
    load(again_hbm, again, in_sem.at[3], 0)
    load(fgain_hbm, fgain, in_sem.at[4], 0)
    load(x_hbm.at[my_rows], xres, in_sem.at[5], 0)

    def w_slot(j):
        return wa.at[:, :, j * COL:(j + 1) * COL]

    load(wq_hbm.at[:, :, cols(side * q_cols, COL)], w_slot(0), w_sem.at[0])
    load(wq_hbm.at[:, :, cols(side * q_cols + COL, COL)], w_slot(1), w_sem.at[1])
    load(wkv_hbm.at[:, :, cols(side * head, COL)], w_slot(2), w_sem.at[2])
    load(wkv_hbm.at[:, :, cols(kv_half + side * head, COL)], w_slot(3), w_sem.at[3])
    phase('wait_x')
    for i, ref in enumerate((act, lens, freqs, again, fgain, xres)):
        landed(ref, in_sem.at[i])
    by_distance = sorted(range(1, n_x), key=lambda r: (-min(r, n_x - r), r)) + [0]

    def cache_rows(r):
        return pl.ds(lax.rem(chip + r, n_x) * rows, rows)

    def load_cache(r):
        at = cache_rows(r)
        group = by_distance.index(r)
        load(k_hbm.at[at, side], kbuf.at[at], kv_sem.at[group])
        load(v_hbm.at[at, side], vbuf.at[at], kv_sem.at[group])

    order = [0] + by_distance[:-1]

    def slot(r):
        start = order.index(r) * q_cols
        return slice(start, start + q_cols)

    def wo_slot(r):
        return wo.at[slot(r)]

    def load_wo(r):
        src_core = core if r == 0 else 1 - core
        load(wo_hbm.at[CORES * lax.rem(chip + n_x - r, n_x) + src_core], wo_slot(r), wo_sem.at[min(order.index(r), 2)])

    load_cache(by_distance[0])
    phase('tables')
    row_id = lax.broadcasted_iota(jnp.int32, (seqs, seqs), 0)
    col_id = lax.broadcasted_iota(jnp.int32, (seqs, seqs), 1)
    wide = jnp.broadcast_to(lens[...].astype(F32), (seqs, seqs))
    len_col = jnp.sum(jnp.where(row_id == col_id, wide, 0.0), axis=1, keepdims=True)
    angle = len_col * freqs[...]
    cos_part = jnp.cos(angle)
    sin_part = jnp.sin(angle)

    def rotate(vecs):
        first, second = vecs[:, :head // 2], vecs[:, head // 2:]
        return jnp.concatenate([first * cos_part - second * sin_part, second * cos_part + first * sin_part], axis=1)

    phase('norm1')
    inv = rms_scale(square_sums([act[:, i * COL:(i + 1) * COL].astype(F32) for i in range(2 * n_col)]), width)
    for i in range(2 * n_col):
        part = slice(i * COL, (i + 1) * COL)
        act[:, part] = (act[:, part].astype(F32) * inv * again[:, part]).astype(BF16)

    phase('qkv')
    lenc[...] = len_col

    for j in range(4):
        landed(w_slot(0), w_sem.at[j])
        if j:
            load_cache(by_distance[j])
        yb[j] = dot(act[...], wa[:, :, cols(j * COL, COL)].reshape(prow * pcol, COL))

    load_wo(0)
    load_wo(order[1])
    phase('rope')
    for j in range(4):
        vecs = yb[j] if j == 3 else rotate(yb[j])
        yb[j] = vecs.astype(BF16).astype(F32)

    span = kbuf.shape[1]
    keys = 8 * span
    scale = head ** -0.5
    groups = rows // 8
    row = lax.broadcasted_iota(jnp.int32, (2 * rows, keys), 0)
    key = lax.broadcasted_iota(jnp.int32, (2 * rows, keys), 1)
    offset = key - lax.rem(row, 8) * span

    def cat(parts):
        return parts[0] if len(parts) == 1 else jnp.concatenate(parts, axis=0)

    def attend(theres):
        ats = [pl.ds(pl.multiple_of(there * rows, rows), rows) for there in theres]
        q0, q1, k_new, v_new = (cat([yb[j, at, :] for at in ats]) for j in range(4))
        q_pair = pair_blocks(q0, q1).astype(BF16)
        self_score = pair_blocks(jnp.sum(q0 * k_new, axis=1, keepdims=True),
                                 jnp.sum(q1 * k_new, axis=1, keepdims=True)) * scale
        lengths = cat([lenc[at, :] for at in ats])
        len_rows = pair_blocks(lengths, lengths).astype(jnp.int32)
        blocks = [there * rows + 8 * b for there in theres for b in range(groups)]
        scores = cat([
            lax.dot_general(q_pair[16 * n:16 * n + 16], kbuf[pl.ds(b, 8)].reshape(keys, head),
                            (((1,), (1,)), ((), ())), preferred_element_type=F32)
            for n, b in enumerate(blocks)])
        offsets = cat([offset] * len(theres))
        scores = jnp.where((offsets >= 0) & (offsets < len_rows), scores * scale, NEG)
        row_max = jnp.maximum(jnp.max(scores, axis=1, keepdims=True), self_score)
        exp_scores = jnp.exp(scores - row_max)
        self_exp = jnp.exp(self_score - row_max)
        total = jnp.sum(exp_scores, axis=1, keepdims=True) + self_exp
        probs = exp_scores.astype(BF16)
        mixed = cat([dot(probs[16 * n:16 * n + 16], vbuf[pl.ds(b, 8)].reshape(keys, head))
                     for n, b in enumerate(blocks)])
        mixed = mixed + self_exp.astype(BF16).astype(F32) * pair_blocks(v_new, v_new)
        mixed = (mixed / total).reshape(len(blocks), 16, head)
        first = mixed[:, :8].reshape(len(theres) * rows, head).astype(BF16)
        second = mixed[:, 8:].reshape(len(theres) * rows, head).astype(BF16)
        for n, at in enumerate(ats):
            osend[at, :head] = first[n * rows:(n + 1) * rows]
            osend[at, head:] = second[n * rows:(n + 1) * rows]
        return ats

    def send(src, dst, send_sem, recv_sem, where):
        pltpu.make_async_remote_copy(src, dst, send_sem, recv_sem, device_id=where, device_id_type=MESH).start()

    def arrived(dst, sem):
        pltpu.make_async_copy(dst, dst, sem).wait()

    def og_slot(r):
        return og.at[:, slot(r)]

    pl.semaphore_wait(barrier, len(peers))
    for group, pair in enumerate([[r] for r in by_distance]):
        phase('wait_kv%d' % pair[0])
        landed(kbuf.at[pl.ds(0, 2 * len(pair) * rows)], kv_sem.at[group])
        phase('attend%d' % pair[0])
        ats = attend([lax.rem(chip + r, n_x) for r in pair])
        for r, at in zip(pair, ats):
            if r:
                send(osend.at[at], og_slot(r), a2a_send.at[0], a2a_recv.at[min(order.index(r), 2)], on_x(r))
        if pair[0] == by_distance[0]:
            for other in order[2:]:
                load_wo(other)

    phase('loads2')
    seg = ((0, kq), (half // pcol, kq), (kq, half // pcol - kq), (half // pcol + kq, half // pcol - kq))

    def load_gate_up(part):
        for i in (2 * part, 2 * part + 1):
            first, count = seg[i]
            at = pl.ds(first, count)
            for m, (w_hbm, w_buf, tail) in enumerate(((wg_hbm, wg, kbuf), (wu_hbm, wu, vbuf))):
                load(w_hbm.at[at, :, cols(core * half, n_main * COL)], w_buf.at[at], gu_sem.at[m, part])
                for t in range(n_tail):
                    load(w_hbm.at[at, :, cols(core * half + (n_main + t) * COL, COL)],
                         tail.at[pl.ds(t * prow + first, count)], tail_sem.at[m, part])

    load_gate_up(0)
    load_gate_up(1)
    phase('proj')
    def tall_dot(lhs, rhs):
        return dot(jnp.concatenate([lhs] * 4, axis=0), rhs)[:rows]

    phase('proj0')
    landed(wo_slot(0), wo_sem.at[0])
    pp[...] = dot(osend[my_rows, :], wo[0:q_cols, :])
    rest = slice(2 * q_cols, n_x * q_cols)
    phase('proj1')
    landed(wo_slot(order[1]), wo_sem.at[1])
    arrived(og_slot(order[1]), a2a_recv.at[1])
    pp[...] += tall_dot(og[:, slot(order[1])], wo[slot(order[1]), :])
    phase('wait_proj')
    landed(wo.at[rest], wo_sem.at[2])
    arrived(og.at[:, rest], a2a_recv.at[2])
    phase('proj_rest')
    for i, part in enumerate(spans):
        pp[:, part] += tall_dot(og[:, 2 * q_cols:], wo[2 * q_cols:, part])
        send(pp.at[:, part], precv.at[:, part], pp_send.at[0], pp_recv.at[i], mate)
    for j in range(n_col):
        load(wd_hbm.at[:, :, cols(core * half + j * COL, COL)], wa.at[:, :, j * COL:(j + 1) * COL], wd_sem.at[0])

    phase('wait_mate')
    dev_rows = pl.ds(pl.multiple_of(dev * rows, rows), rows)
    for i, part in enumerate(spans):
        arrived(precv.at[:, part], pp_recv.at[i])
        x1b[:, part] = (xres[:, part].astype(F32) + (pp[:, part] + precv[:, part])).astype(BF16)
    phase('norm2')
    inv2 = rms_scale(square_sums([x1b[:, i * COL:(i + 1) * COL].astype(F32) for i in range(2 * n_col)]), width)
    for i in range(2 * n_col):
        part = slice(i * COL, (i + 1) * COL)
        hg[dev_rows, part] = (x1b[:, part].astype(F32) * inv2 * fgain[:, part]).astype(BF16)

    phase('gather')
    ka = kq * pcol // 2
    kb = (half - kq * pcol) // 2
    strips = (((0, ka), (ka, ka)), ((2 * ka, kb), (2 * ka + kb, kb)))

    def piece(owner, strip, whose):
        owner_rows = pl.ds(pl.multiple_of(lax.rem(owner + 2 * n_dev, n_dev) * rows, rows), rows)
        return hg.at[owner_rows, cols(whose * half + strip[0], strip[1])]

    def across(step):
        return {**on_y(step), **mate}

    kind = (0, 1, 2, 2, 3, 3) + (4,) * 6

    def hop(owner, strip, p, i, where, whose):
        ref = piece(owner, strip, whose)
        send(ref, ref, ag_send.at[0], ag_recv.at[p, kind[i]], where)

    source = ((-1, 0), (1, 1), (-1, 1), (1, 0), (2, 0), (2, 1))
    def hop_own(p, late):
        if late:
            hop(dev, strips[p][1], p, 2, across(1), core)
            hop(dev, strips[p][0], p, 3, across(-1), core)
        else:
            hop(dev, strips[p][0], p, 0, across(1), core)
            hop(dev, strips[p][1], p, 1, across(-1), core)

    hop_own(0, False)
    hop_own(0, True)
    hop_own(1, False)

    def take_near(p, i):
        owner = dev + 2 * i - 1
        start = strips[p][0][0] + i * strips[p][0][1]
        ref = piece(owner, (start, strips[p][0][1]), 1 - core)
        arrived(ref, ag_recv.at[p, i])
        send(ref, ref, ag_send.at[0], ag_recv.at[p, 3], across(1 - 2 * i))
        send(ref, ref, ag_send.at[0], ag_recv.at[p, 4], mate)

    def both(p, count):
        return hg.at[0:rows, 0:count * strips[p][0][1]]

    def take_pair(p, first):
        arrived(both(p, 2), ag_recv.at[p, kind[first]])
        for i in (first, first + 1):
            owner, strip = dev + source[i][0], strips[p][source[i][1]]
            hop(owner, strip, p, 6 + i, mate, 1 - core if i < 4 else core)

    def from_mate(p):
        arrived(both(p, 6), ag_recv.at[p, 4])

    def weights(m, j, i):
        first, count = seg[i]
        main, tail = (wg, kbuf) if m == 0 else (wu, vbuf)
        if isinstance(j, int) and j >= n_main:
            start = (j - n_main) * prow + first
            return tail[start:start + count].reshape(count * pcol, COL)
        return main[first:first + count, :, cols(j * COL, COL)].reshape(count * pcol, COL)

    def partial_sum(m, j, p):
        out = None
        for i in (2 * p, 2 * p + 1):
            first, count = seg[i]
            term = dot(hg[:, first * pcol:(first + count) * pcol], weights(m, j, i))
            out = term if out is None else out + term
        return out

    def gate_up(p, group):
        for j in group:
            gate, up = partial_sum(0, j, p), partial_sum(1, j, p)
            if p == 0:
                yb[j] = gate
                ub[j] = up
            else:
                gate = yb[j] + gate
                gate = 0.5 * gate * (1.0 + jnp.tanh(0.5 * gate))
                u[:, cols(core * half + j * COL, COL)] = (gate * (ub[j] + up)).astype(BF16)
        if p == 1:
            for j in group:
                here = u.at[:, cols(core * half + j * COL, COL)]
                send(here, here, u_send.at[0], u_recv.at[0], mate)

    def gate_up_part(p):
        count = seg[2 * p][1]
        for m, (w_buf, tail) in enumerate(((wg, kbuf), (wu, vbuf))):
            landed(w_buf.at[pl.ds(0, 2 * count)], gu_sem.at[m, p])
            landed(tail.at[pl.ds(0, 2 * n_tail * count)], tail_sem.at[m, p])
        phase('gateup%d' % p)

        if p == 0:
            gate_up(p, range(n_col - 4))
            phase('gather2')
            take_pair(1, 2)
            take_pair(1, 4)
            phase('gateup0b')
            gate_up(p, range(n_col - 4, n_col))
        else:
            gate_up(p, range(n_col - 2))
            gate_up(p, range(n_col - 2, n_col))

    near = 1 - jnp.minimum(dev, 1)
    take_near(0, near)
    take_near(0, 1 - near)
    hop_own(1, True)
    phase('gather_b')
    take_pair(0, 2)
    take_near(1, near)
    take_near(1, 1 - near)
    phase('gather_c')
    take_pair(0, 4)
    from_mate(0)
    phase('wait_gu0')
    gate_up_part(0)
    phase('gather3')
    from_mate(1)
    phase('wait_gu1')
    gate_up_part(1)
    phase('down0')
    fold_half = half // pcol

    def down_half(whose, group):
        at = pl.ds(whose * fold_half, fold_half)
        part = slice(group[0] * COL, (group[-1] + 1) * COL)
        return dot(u[:, cols(whose * half, half)], wa[at, :, part].reshape(half, len(group) * COL))

    def keep(group, value, add):
        for n, j in enumerate(group):
            piece_of = value[:, n * COL:(n + 1) * COL]
            yb[j] = yb[j] + piece_of if add else piece_of

    pairs = [range(max(j - 1, 0), j + 1) for j in range(0, n_col, 2)]
    landed(wa, wd_sem.at[0])
    for group in pairs[:2]:
        keep(group, down_half(core, group), False)

    phase('wait_u')
    arrived(u.at[:, cols((1 - core) * half, half)], u_recv.at[0])

    phase('down')
    def way(j):
        sign = (1 - 2 * core) * (1 - 2 * (j % 2))
        return sign

    def rows_of(owner):
        return pl.ds(pl.multiple_of(lax.rem(owner + 2 * n_dev, n_dev) * rows, rows), rows)

    blk = rows // CORES
    sides = [{'side': CORES * chip + b} for b in range(CORES)]

    def block_of(owner, b):
        start = lax.rem(owner + 2 * n_dev, n_dev) * rows + b * blk
        return pl.ds(pl.multiple_of(start, blk), blk)

    def pass_far(j):
        send(yb.at[j, rows_of(dev + 2)], r1.at[j], rs_send.at[0], far_recv.at[j], on_y(way(j)))

    def pass_near(j):
        sign = way(j)
        for b in range(CORES):
            send(yb.at[j, block_of(dev - sign, b)], r3.at[core, j], rs_send.at[2], rs_recv.at[1],
                 {**on_y(-sign), **sides[b]})

    def pass_sum(j):
        sign = way(j)
        arrived(r1.at[j], far_recv.at[j])
        yb[j, rows_of(dev + sign), :] += r1[j]
        for b in range(CORES):
            send(yb.at[j, block_of(dev + sign, b)], r2.at[core, j], rs_send.at[1], rs_recv.at[0],
                 {**on_y(sign), **sides[b]})

    for group in pairs:
        if group in pairs[:2]:
            keep(group, down_half(1 - core, group), True)
        else:
            part = slice(group[0] * COL, (group[-1] + 1) * COL)
            keep(group, dot(u[...], wa[:, :, part].reshape(prow * pcol, len(group) * COL)), False)
        for j in group:
            pass_far(j)

    phase('stage2')
    for j in range(n_col):
        pass_near(j)
    for j in range(n_col):
        send(yb.at[j, block_of(dev, 1 - core)], r4.at[j], fin_send.at[0], fin_recv.at[0], mate)
    for j in range(n_col):
        pass_sum(j)

    phase('final')
    my_blk = pl.ds(pl.multiple_of(core * blk, blk), blk)

    def finish(whose, j, own_sum):
        y = (own_sum + r2[whose, j] + r3[whose, j]).astype(BF16)
        here = cols(whose * half + j * COL, COL)
        out[:, here] = (x1b[my_blk, here].astype(F32) + y.astype(F32)).astype(BF16)

    arrived(r4, fin_recv.at[0])
    arrived(r3, rs_recv.at[1])
    arrived(r2, rs_recv.at[0])
    for j in range(n_col):
        finish(core, j, yb[j, block_of(dev, core), :])
        finish(1 - core, j, r4[j])
    phase('drain')
    arrived(og.at[:, q_cols:], a2a_send.at[0])
    arrived(pp, pp_send.at[0])
    arrived(hg.at[0:(CORES + 1) * rows], ag_send.at[0])
    arrived(u.at[:, cols(core * half, half)], u_send.at[0])
    arrived(r1, rs_send.at[0])
    arrived(r2, rs_send.at[1])
    arrived(r3, rs_send.at[2])
    arrived(r4, fin_send.at[0])
    phase(None)


def solution(mesh):
    n_side = mesh.shape['side']
    n_dev = mesh.shape['dev']
    batch_axes = ('inst', 'dev')
    in_specs = (
        P(batch_axes, None),
        P(batch_axes),
        P(None, batch_axes, None, None, None),
        P(None, batch_axes, None, None, None),
        P(), P(), P(), P(), P(),
        P(None, None, 'dev'),
        P(None, None, 'dev'),
        P(None, 'dev', None),
    )
    out_specs = P(('inst', 'dev', 'side'), None)

    def device_fn(hidden, cache_len, k_cache, v_cache, w_q, w_kv, w_o, attn_gain, ffn_gain, w_gate, w_up, w_down):
        seqs, width = hidden.shape
        span, head = k_cache.shape[3:]
        ff = w_gate.shape[2]
        half = width // 2
        rows = seqs * CORES // n_side
        n_x = n_side // CORES
        n_col = half // COL
        q_cols = w_q.shape[2] // n_side
        tall = width // span
        freqs = jnp.asarray(ROPE_BASE ** (-np.arange(head // 2, dtype=np.float64) / (head // 2)), F32)[None]

        def fold(w):
            return w.reshape(w.shape[1] // span, span, w.shape[2])

        args = (hidden, cache_len.reshape(1, seqs), freqs, k_cache[0], v_cache[0], fold(w_q), fold(w_kv),
                w_o.reshape(n_side, w_o.shape[1] // n_side, width), attn_gain, ffn_gain,
                fold(w_gate), fold(w_up), fold(w_down))
        vmem = pltpu.VMEM
        dma = pltpu.SemaphoreType.DMA
        main = ff // CORES - 2 * COL
        scratch = [
            vmem((seqs, width), BF16), vmem((1, seqs), jnp.int32), vmem((1, head // 2), F32),
            vmem((1, width), F32), vmem((1, width), F32), vmem((rows, width), BF16),
            vmem((tall, span, half), BF16),
            vmem((seqs, span, head), BF16), vmem((seqs, span, head), BF16),
            vmem((n_x * q_cols, width), BF16),
            vmem((tall, span, main), BF16), vmem((tall, span, main), BF16),
            vmem((n_col, seqs, COL), F32), vmem((n_col, seqs, COL), F32), vmem((seqs, 1), F32),
            vmem((seqs, q_cols), BF16), vmem((rows, n_x * q_cols), BF16),
            vmem((rows, width), F32), vmem((rows, width), F32), vmem((rows, width), BF16),
            vmem((n_dev * rows, width), BF16), vmem((seqs, ff), BF16),
            vmem((n_col, rows, COL), F32), vmem((CORES, n_col, rows // CORES, COL), F32),
            vmem((CORES, n_col, rows // CORES, COL), F32), vmem((n_col, rows // CORES, COL), F32),
            dma((6,)), dma((4,)), dma((n_x,)), dma((3,)), dma((2, 2)), dma((2, 2)), dma((1,)),
            dma((1,)), dma((3,)), dma((1,)), dma((2,)), dma((1,)), dma((2, 5)), dma((1,)), dma((1,)),
            dma((3,)), dma((2,)), dma((n_col,)), dma((1,)), dma((1,)),
        ]
        anywhere = pl.BlockSpec(memory_space=pl.ANY)
        return pl.pallas_call(
            functools.partial(layer_kernel, n_dev, n_side),
            out_shape=jax.ShapeDtypeStruct((rows // CORES, width), BF16),
            in_specs=[anywhere] * len(args),
            out_specs=pl.BlockSpec(memory_space=pltpu.VMEM),
            scratch_shapes=scratch,
            compiler_params=pltpu.CompilerParams(
                collective_id=0, has_side_effects=True, vmem_limit_bytes=67_043_328),
        )(*args)

    return jax.shard_map(device_fn, mesh=mesh, in_specs=in_specs, out_specs=out_specs, check_vma=False)
```
